256 devices in a mesh: job: 4 (over x), zero: 16 (over z, core), cols: 4 (over y).
Axes of the slice: x: 4, y: 4, z: 8, core: 2. Of those that a mesh axis runs over, the one named last changes fastest.
Arguments:
- weight_gate: bfloat16 [8192, 8192], P(('job', 'zero'), 'cols'), parts along dimension 0, may hold values from -0.1875 to 0.1875
- low_gate: bfloat16 [8192, 32], P(('job', 'zero')), parts along dimension 0, may hold values from -0.125 to 0.125
- high_gate: bfloat16 [128, 8192], P('job', 'cols'), parts along dimension 0, may hold values from -1 to 1
- weight_up: bfloat16 [8192, 8192], P(('job', 'zero'), 'cols'), parts along dimension 0, may hold values from -0.1875 to 0.1875
- low_up: bfloat16 [8192, 32], P(('job', 'zero')), parts along dimension 0, may hold values from -0.125 to 0.125
- high_up: bfloat16 [128, 8192], P('job', 'cols'), parts along dimension 0, may hold values from -1 to 1
- norm_train: float32 [8192], P(('job', 'zero', 'cols')), parts along dimension 0, may hold values from 0.25 to 1.75
- norm_step: float32 [8192], P(('job', 'zero', 'cols')), parts along dimension 0, may hold values from -0.3 to 0.3
Outputs:
- serving_gate: bfloat16 [8192, 8192], P('job', 'cols'), parts along dimension 0
- serving_up: bfloat16 [8192, 8192], P('job', 'cols'), parts along dimension 0
- column_gate: float32 [32768], P(('job', 'cols')), parts along dimension 0
- column_up: float32 [32768], P(('job', 'cols')), parts along dimension 0
- serve_norm: bfloat16 [8192], P('job'), parts along dimension 0
The draws below stay inside these ranges and needn't reach their ends.
There are 4 independent parts, one for each index of `job`. The reference program is written for one: setup_inputs(seed, part) draws one part's arguments, and reference() takes and returns one part's arrays. A program takes and returns all parts, laid end to end along the dimension named above; each array names one. Nothing has to cross between parts.
All inputs are finite; a program needn't handle non-finite values. Where the reference program divides by a largest or mean magnitude, that divisor is 1e-20 or more.
Results may differ from the reference program's by a relative error of at most 0.001.
Values may be sent and summed in bfloat16 or wider, within the bound.
A program may use at most 128 MiB of HBM per device.

```python
import jax
import jax.numpy as jnp

D_MODEL = 2048
D_INNER = 8192
RANK = 32


def raised(array, own_key, source, target, blocks, factor):
    def block_of(position):
        return (jnp.arange(array.shape[position]) // (array.shape[position] // blocks)).reshape((-1,) + (1,) * (array.ndim - 1 - position))

    one_side = jax.random.permutation(own_key, blocks)[block_of(target)]
    second = (block_of(target) + blocks // 2) % blocks
    return jnp.where((block_of(source) == one_side) | (block_of(source) == second), factor * array, array)


def level_of(key, dims, pieces, smallest, largest):
    def one(position, shards_of):
        draws = jax.random.uniform(jax.random.fold_in(jax.random.fold_in(key, 6), position), (shards_of,), jnp.float32, smallest / len(pieces), largest / len(pieces))
        return jnp.repeat(jnp.exp(draws), dims[position] // shards_of).reshape((-1,) + (1,) * (len(dims) - position - 1))

    level = one(*pieces[0])
    for cut in pieces[1:]:
        level = level * one(*cut)
    return level


def normal_values(rng, dims, scale, bound, pieces=(), dtype=jnp.bfloat16):
    entries = scale * jax.random.normal(rng, dims, jnp.float32)
    if pieces:
        entries = entries * level_of(rng, dims, pieces, -0.22, 0.18)
    return jnp.clip(entries, -bound, bound).astype(dtype)


def gaussian_with(own_key, dims, deviation, most, split, heavy, held_as=jnp.bfloat16):
    array = deviation * jax.random.normal(own_key, dims, jnp.float32)
    if split:
        array = array * level_of(own_key, dims, split, -0.22, 0.18)
    return jnp.clip(raised(array, jax.random.fold_in(own_key, 3), *heavy), -most, most).astype(held_as)


def setup_inputs(seed: int = 0, part: int = 0) -> dict:
    keys = jax.random.split(jax.random.key(seed), 9)
    part_keys = jax.random.split(jax.random.fold_in(keys[8], part), 9)
    weight_gate = gaussian_with(part_keys[0], (D_MODEL, D_INNER), D_MODEL ** -0.5, 0.1875, ((0, 16), (1, 4)), (0, 1, 16, 2.0))
    low_gate = normal_values(part_keys[1], (D_MODEL, RANK), D_MODEL ** -0.5, 0.125, ((0, 16),))
    high_gate = normal_values(part_keys[2], (RANK, D_INNER), RANK ** -0.5, 1.0, ((1, 4),))
    weight_up = gaussian_with(part_keys[3], (D_MODEL, D_INNER), D_MODEL ** -0.5, 0.1875, ((0, 16), (1, 4)), (0, 1, 16, 2.0))
    low_up = normal_values(part_keys[4], (D_MODEL, RANK), D_MODEL ** -0.5, 0.125, ((0, 16),))
    high_up = normal_values(part_keys[5], (RANK, D_INNER), RANK ** -0.5, 1.0, ((1, 4),))
    norm_train = jnp.clip(1.0 + 0.15 * jax.random.normal(part_keys[6], (D_MODEL,), jnp.float32), 0.25, 1.75)
    norm_step = jnp.clip(jax.random.uniform(part_keys[7], (D_MODEL,), jnp.float32, -0.3, 0.3) * level_of(part_keys[7], (D_MODEL,), ((0, 64),), -0.4, 0.0), -0.3, 0.3)
    return {"weight_gate": weight_gate, "low_gate": low_gate, "high_gate": high_gate, "weight_up": weight_up, "low_up": low_up, "high_up": high_up, "norm_train": norm_train, "norm_step": norm_step}


mix_rate = 2.0


def reference(weight_gate, low_gate, high_gate, weight_up, low_up, high_up, norm_train, norm_step):
    whole_gate = weight_gate.astype(jnp.float32) + mix_rate * jnp.dot(low_gate, high_gate, preferred_element_type=jnp.float32)
    whole_up = weight_up.astype(jnp.float32) + mix_rate * jnp.dot(low_up, high_up, preferred_element_type=jnp.float32)
    column_gate = jnp.max(jnp.abs(whole_gate), axis=0)
    serving_gate = (whole_gate / column_gate).astype(jnp.bfloat16)
    column_up = jnp.max(jnp.abs(whole_up), axis=0)
    serving_up = (whole_up / column_up).astype(jnp.bfloat16)
    serve_norm = (norm_train + norm_step).astype(jnp.bfloat16)
    return serving_gate, serving_up, column_gate, column_up, serve_norm
```

```python
import functools

import jax
import jax.numpy as jnp
from jax import lax
from jax.experimental import pallas as pl
from jax.experimental.pallas import tpu as pltpu
from jax.sharding import PartitionSpec as P

mix_rate = 2.0
MESH = pl.DeviceIdType.MESH
CH = 4
TILE = 512
LANES = 128


def remote(src, dst, send_sem, recv_sem, device_id):
    return pltpu.make_async_remote_copy(
        src_ref=src, dst_ref=dst, send_sem=send_sem, recv_sem=recv_sem, device_id=device_id, device_id_type=MESH
    )


def kernel(
    nz, ny,
    wg_hbm, lg_hbm, hg_hbm, wu_hbm, lu_hbm, hu_hbm, nt_hbm, ns_hbm,
    og, ou, col_out, norm_out,
    w_in, l_in, h_in, n_in, whole, pmax, pget, cmax, allmax, ybuf, zbuf,
    in_sem, ring_send, ring_recv, pair_send, pair_recv, max_send, max_recv, ny_send, ny_recv, nz_send, nz_recv,
):
    zero, col = lax.axis_index("zero"), lax.axis_index("cols")
    z, core = zero // 2, zero % 2
    outs = (og, ou)
    rows, columns = w_in.shape[1:]
    step_rows = rows // CH

    loads = [
        pltpu.make_async_copy(src, dst, in_sem.at[i])
        for i, (src, dst) in enumerate(
            (
                (lg_hbm, l_in.at[0]), (hg_hbm, h_in.at[0]), (wg_hbm, w_in.at[0]),
                (lu_hbm, l_in.at[1]), (hu_hbm, h_in.at[1]), (wu_hbm, w_in.at[1]),
                (nt_hbm, n_in.at[0]), (ns_hbm, n_in.at[1]),
            )
        )
    ]
    for c in loads:
        c.start()

    barrier = pltpu.get_barrier_semaphore()
    peer = zero + 1 - 2 * core
    others = [(z + d) % nz * 2 + core for d in range(1, nz)]
    others_cross = [(z + d) % nz * 2 + 1 - core for d in range(1, nz)]
    for t in others + others_cross + [peer]:
        pl.semaphore_signal(barrier, 1, device_id={"zero": t}, device_id_type=MESH)
    for d in range(1, ny):
        pl.semaphore_signal(barrier, 1, device_id={"cols": (col + d) % ny}, device_id_type=MESH)

    for m in range(2):
        for i in range(3):
            loads[3 * m + i].wait()
        for t in range(columns // TILE):
            at = slice(t * TILE, (t + 1) * TILE)
            new = w_in[m, :, at].astype(jnp.float32) + mix_rate * lax.dot_general(
                l_in[m], h_in[m, :, at], (((0,), (0,)), ((), ())), preferred_element_type=jnp.float32
            )
            whole[m, :, at] = new
            top = jnp.max(jnp.abs(new), axis=0, keepdims=True)
            for q in range(TILE // LANES):
                r = t * (TILE // LANES) + q
                pmax[m, r : r + 1, :] = top[:, q * LANES : (q + 1) * LANES]
    loads[6].wait()
    loads[7].wait()
    gain = n_in[0] + n_in[1]
    ybuf[pl.ds(col, 1)] = jnp.concatenate([gain] * ny, axis=1)[None]

    pl.semaphore_wait(barrier, 2 * nz - 1 + ny - 1)

    first = remote(pmax.at[1 - core], pget, max_send.at[0], max_recv.at[0], {"zero": peer})
    first.start()
    norm_y = [
        remote(ybuf.at[col], ybuf.at[col], ny_send.at[d - 1], ny_recv.at[d - 1], {"cols": (col + d) % ny})
        for d in range(1, ny)
    ]
    for c in norm_y:
        c.start()
    first.wait_recv()
    cmax[...] = jnp.maximum(pmax[core], pget[...])
    spread = [
        remote(cmax, allmax.at[d], max_send.at[d], max_recv.at[d], {"zero": others[d - 1]}) for d in range(1, nz)
    ]
    for c in spread:
        c.start()
    for c in norm_y:
        c.wait_recv()
    lane = lax.broadcasted_iota(jnp.int32, (1, LANES), 1) // (LANES // ny)
    row = ybuf[0]
    for k in range(1, ny):
        row = jnp.where(lane == k, ybuf[k], row)
    zbuf[pl.ds(zero, 1)] = row[None]
    top = cmax[...]
    for d, c in enumerate(spread):
        c.wait_recv()
        top = jnp.maximum(top, allmax[d + 1])
    col_out[pl.ds(core, 1)] = top[None]
    back = remote(col_out.at[core], col_out.at[core], max_send.at[nz], max_recv.at[nz], {"zero": peer})
    back.start()
    norm_z = [
        remote(zbuf.at[zero], zbuf.at[zero], nz_send.at[i], nz_recv.at[i], {"zero": t})
        for i, t in enumerate(others + others_cross + [peer])
    ]
    for c in norm_z:
        c.start()
    back.wait_recv()

    mine = pl.multiple_of(zero * rows, rows)
    for m in range(2):
        for r in range(columns // LANES):
            at = slice(r * LANES, (r + 1) * LANES)
            inv = 1.0 / col_out[m, r : r + 1, :]
            outs[m][pl.ds(mine, rows), at] = (whole[m, :, at] * inv).astype(jnp.bfloat16)

    to = ((z + 1) % nz * 2 + core, (z + nz - 1) % nz * 2 + core)
    half = nz // 2

    def piece(d, s, k):
        b = (z - s + nz) % nz if d == 0 else (z + s) % nz
        m = k // CH if d == 0 else 1 - k // CH
        at = pl.multiple_of((b * 2 + core) * rows + k % CH * step_rows, step_rows)
        return m, outs[m].at[pl.ds(at, step_rows)]

    def ring(d, s, k):
        _, ref = piece(d, s, k)
        return remote(ref, ref, ring_send.at[d], ring_recv.at[d, s, k], {"zero": to[d]})

    def pair(d, s, k):
        m, ref = piece(d, s, k)
        slot = s if d == m else (nz - s) % nz
        return remote(ref, ref, pair_send, pair_recv.at[m, slot], {"zero": peer})

    for k in range(2 * CH):
        for d in range(2):
            ring(d, 0, k).start()
    for k in range(2 * CH):
        pair(0, 0, k).start()
    for s in range(1, half + 1):
        for k in range(2 * CH if s < half else CH):
            for d in range(2):
                ring(d, s - 1, k).wait_recv()
                if s < half - 1 or s == half - 1 and k < CH:
                    ring(d, s, k).start()
                pair(d, s, k).start()

    for c in norm_z:
        c.wait_recv()
    norm_out[...] = zbuf[:, 0, :]
    for m in range(2):
        for slot in range(nz):
            block = outs[m].at[pl.ds(0, rows)]
            remote(block, block, pair_send, pair_recv.at[m, slot], {"zero": peer}).wait_recv()
    total = og.at[pl.ds(0, rows * (nz - 1))]
    for d in range(2):
        remote(total, total, ring_send.at[d], ring_recv.at[d, 0, 0], {"zero": to[d]}).wait_send()
    remote(og, og, pair_send, pair_recv.at[0, 0], {"zero": peer}).wait_send()
    for c in [first, *norm_y, *spread, back, *norm_z]:
        c.wait_send()


def per_device(weight_gate, low_gate, high_gate, weight_up, low_up, high_up, norm_train, norm_step):
    devices, ny = lax.axis_size("zero"), lax.axis_size("cols")
    nz = devices // 2
    rows, columns = weight_gate.shape
    rank = low_gate.shape[1]
    share = norm_train.shape[0]
    tiles = columns // LANES
    f32, bf16 = jnp.float32, jnp.bfloat16
    hbm = pl.BlockSpec(memory_space=pltpu.HBM)
    vmem = pl.BlockSpec(memory_space=pltpu.VMEM)
    dma = pltpu.SemaphoreType.DMA
    serving_gate, serving_up, column, norm = pl.pallas_call(
        functools.partial(kernel, nz, ny),
        out_shape=(
            pltpu.VMEM((devices * rows, columns), bf16),
            pltpu.VMEM((devices * rows, columns), bf16),
            pltpu.VMEM((2, tiles, LANES), f32),
            pltpu.VMEM((devices, LANES), f32),
        ),
        in_specs=[hbm] * 8,
        out_specs=(vmem,) * 4,
        scratch_shapes=[
            pltpu.VMEM((2, rows, columns), bf16),
            pltpu.VMEM((2, rank, rows), bf16),
            pltpu.VMEM((2, rank, columns), bf16),
            pltpu.VMEM((2, 1, share), f32),
            pltpu.VMEM((2, rows, columns), f32),
            pltpu.VMEM((2, tiles, LANES), f32),
            pltpu.VMEM((tiles, LANES), f32),
            pltpu.VMEM((tiles, LANES), f32),
            pltpu.VMEM((nz, tiles, LANES), f32),
            pltpu.VMEM((ny, 1, LANES), f32),
            pltpu.VMEM((devices, 1, LANES), f32),
            dma((8,)),
            dma((2,)),
            dma((2, nz // 2, 2 * CH)),
            dma,
            dma((2, nz)),
            dma((nz + 1,)),
            dma((nz + 1,)),
            dma((max(ny - 1, 1),)),
            dma((max(ny - 1, 1),)),
            dma((devices - 1,)),
            dma((devices - 1,)),
        ],
        compiler_params=pltpu.CompilerParams(
            collective_id=0, has_side_effects=True, vmem_limit_bytes=47 << 20
        ),
    )(
        weight_gate, low_gate.T, high_gate, weight_up, low_up.T, high_up,
        norm_train.reshape(1, share), norm_step.reshape(1, share),
    )
    column = column.reshape(2, columns)
    return (serving_gate, serving_up, column[0], column[1], norm.reshape(-1).astype(bf16))


def solution(mesh):
    in_specs = (
        P(("job", "zero"), "cols"),
        P(("job", "zero"), None),
        P("job", "cols"),
        P(("job", "zero"), "cols"),
        P(("job", "zero"), None),
        P("job", "cols"),
        P(("job", "zero", "cols")),
        P(("job", "zero", "cols")),
    )
    out_specs = (
        P("job", "cols"),
        P("job", "cols"),
        P(("job", "cols")),
        P(("job", "cols")),
        P("job"),
    )
    return jax.shard_map(
        per_device, mesh=mesh, in_specs=in_specs, out_specs=out_specs, check_vma=False
    )
```

```python
import functools

import jax
import jax.numpy as jnp
from jax import lax
from jax.experimental import pallas as pl
from jax.experimental.pallas import tpu as pltpu
from jax.sharding import PartitionSpec as P

mix_rate = 2.0
MESH = pl.DeviceIdType.MESH
CH = 4
TILE = 512
DEPTH = 4
LANES = 128


def remote(src, dst, send_sem, recv_sem, device_id):
    return pltpu.make_async_remote_copy(
        src_ref=src, dst_ref=dst, send_sem=send_sem, recv_sem=recv_sem, device_id=device_id, device_id_type=MESH
    )


def kernel(
    nz, ny,
    wg_hbm, lg_hbm, hg_hbm, wu_hbm, lu_hbm, hu_hbm, nt_hbm, ns_hbm,
    og, ou, col_out, norm_out,
    w_in, l_in, h_in, n_in, raw, l_raw, whole, pmax, pget, cmax, allmax, inv, ybuf, zbuf,
    in_sem, ring_send, ring_recv, low_send, low_recv, pair_send, pair_recv,
    max_send, max_recv, ny_send, ny_recv, nz_send, nz_recv,
):
    zero, col = lax.axis_index("zero"), lax.axis_index("cols")
    z, core = zero // 2, zero % 2
    outs = (og, ou)
    rows, columns = w_in.shape[1:]
    step_rows = rows // CH
    half = nz // 2
    pieces = (2 * half - 1) * CH

    loads = [
        pltpu.make_async_copy(src, dst, in_sem.at[i])
        for i, (src, dst) in enumerate(
            (
                (lg_hbm, l_in.at[0]), (hg_hbm, h_in.at[0]), (wg_hbm, w_in.at[0]),
                (lu_hbm, l_in.at[1]), (hu_hbm, h_in.at[1]), (wu_hbm, w_in.at[1]),
                (nt_hbm, n_in.at[0]), (ns_hbm, n_in.at[1]),
            )
        )
    ]
    for c in loads:
        c.start()

    barrier = pltpu.get_barrier_semaphore()
    peer = zero + 1 - 2 * core
    others = [(z + d) % nz * 2 + core for d in range(1, nz)]
    others_cross = [(z + d) % nz * 2 + 1 - core for d in range(1, nz)]
    for t in others + others_cross + [peer]:
        pl.semaphore_signal(barrier, 1, device_id={"zero": t}, device_id_type=MESH)
    for d in range(1, ny):
        pl.semaphore_signal(barrier, 1, device_id={"cols": (col + d) % ny}, device_id_type=MESH)

    def merged(weights, low, m, at):
        return weights[:, at].astype(jnp.float32) + mix_rate * lax.dot_general(
            low[...], h_in[m, :, at], (((0,), (0,)), ((), ())), preferred_element_type=jnp.float32
        )

    for m in range(2):
        for i in range(3):
            loads[3 * m + i].wait()
        for t in range(columns // TILE):
            at = slice(t * TILE, (t + 1) * TILE)
            new = merged(w_in.at[m], l_in.at[m], m, at)
            whole[m, :, at] = new
            top = jnp.max(jnp.abs(new), axis=0, keepdims=True)
            for q in range(TILE // LANES):
                r = t * (TILE // LANES) + q
                pmax[m, r : r + 1, :] = top[:, q * LANES : (q + 1) * LANES]
    loads[6].wait()
    loads[7].wait()
    gain = n_in[0] + n_in[1]
    ybuf[pl.ds(col, 1)] = jnp.concatenate([gain] * ny, axis=1)[None]

    to = ((z + 1) % nz * 2 + core, (z + nz - 1) % nz * 2 + core)

    def block_rows(d, s):
        b = (z - s + nz) % nz if d == 0 else (z + s) % nz
        return (b * 2 + core) * rows

    def piece(d, i, hops):
        k = i % (2 * CH)
        m = k // CH if d == 0 else 1 - k // CH
        at = pl.multiple_of(block_rows(d, i // (2 * CH) + hops) + k % CH * step_rows, step_rows)
        return m, outs[m].at[pl.ds(at, step_rows)]

    def ring(d, i):
        if i < CH:
            at = pl.ds(i * step_rows, step_rows)
            src, dst = w_in.at[d, at], raw.at[d, at]
        else:
            _, src = piece(d, i, 0)
            dst = src
        return remote(src, dst, ring_send.at[d, i % DEPTH], ring_recv.at[d, i], {"zero": to[d]})

    def pair(d, i):
        m, ref = piece(d, i, 1)
        s = i // (2 * CH) + 1
        slot = s if d == m else (nz - s) % nz
        return remote(ref, ref, pair_send, pair_recv.at[m, slot], {"zero": peer})

    def low(d):
        return remote(l_in.at[d], l_raw.at[d], low_send.at[d], low_recv.at[d], {"zero": to[d]})

    pl.semaphore_wait(barrier, 2 * nz - 1 + ny - 1)

    first = remote(pmax.at[1 - core], pget, max_send.at[0], max_recv.at[0], {"zero": peer})
    first.start()
    norm_y = [
        remote(ybuf.at[col], ybuf.at[col], ny_send.at[d - 1], ny_recv.at[d - 1], {"cols": (col + d) % ny})
        for d in range(1, ny)
    ]
    for c in norm_y:
        c.start()
    for d in range(2):
        low(d).start()
        ring(d, 0).start()
    first.wait_recv()
    cmax[...] = jnp.maximum(pmax[core], pget[...])
    spread = [
        remote(cmax, allmax.at[d], max_send.at[d], max_recv.at[d], {"zero": others[d - 1]}) for d in range(1, nz)
    ]
    for c in spread:
        c.start()
    for i in range(1, min(DEPTH, CH)):
        for d in range(2):
            ring(d, i).start()
    for c in norm_y:
        c.wait_recv()
    lane = lax.broadcasted_iota(jnp.int32, (1, LANES), 1) // (LANES // ny)
    row = ybuf[0]
    for k in range(1, ny):
        row = jnp.where(lane == k, ybuf[k], row)
    zbuf[pl.ds(zero, 1)] = row[None]
    top = cmax[...]
    for d, c in enumerate(spread):
        c.wait_recv()
        top = jnp.maximum(top, allmax[d + 1])
    col_out[pl.ds(core, 1)] = top[None]
    back = remote(col_out.at[core], col_out.at[core], max_send.at[nz], max_recv.at[nz], {"zero": peer})
    back.start()
    norm_z = [
        remote(zbuf.at[zero], zbuf.at[zero], nz_send.at[i], nz_recv.at[i], {"zero": t})
        for i, t in enumerate(others + others_cross + [peer])
    ]
    for c in norm_z:
        c.start()
    back.wait_recv()
    for m in range(2):
        for r in range(columns // LANES):
            inv[m, :, r * LANES : (r + 1) * LANES] = 1.0 / col_out[m, r : r + 1, :]

    mine = pl.multiple_of(zero * rows, rows)
    for m in range(2):
        for t in range(columns // TILE):
            at = slice(t * TILE, (t + 1) * TILE)
            outs[m][pl.ds(mine, rows), at] = (whole[m, :, at] * inv[m, :, at]).astype(jnp.bfloat16)

    def send(d, i):
        if i >= DEPTH:
            ring(d, i - DEPTH).wait_send()
        ring(d, i).start()

    def receive(d, i):
        ring(d, i).wait_recv()
        pair(d, i).start()

    for i in range(min(DEPTH, CH), pieces):
        if i == CH:
            for m in range(2):
                block = outs[m].at[pl.ds(mine, rows)]
                remote(block, block, pair_send, pair_recv.at[m, 0], {"zero": peer}).start()
        if i == 2 * CH:
            for d in range(2):
                low(d).wait_recv()
                for k in range(CH):
                    ring(d, k).wait_recv()
                near = pl.multiple_of(block_rows(d, 1), rows)
                for t in range(columns // TILE):
                    at = slice(t * TILE, (t + 1) * TILE)
                    new = merged(raw.at[d], l_raw.at[d], d, at) * inv[d, :, at]
                    outs[d][pl.ds(near, rows), at] = new.astype(jnp.bfloat16)
            for d in range(2):
                for k in range(CH):
                    pair(d, k).start()
        for d in range(2):
            send(d, i)
        if i >= CH + DEPTH:
            for d in range(2):
                receive(d, i - DEPTH)
    for i in range(pieces - DEPTH, pieces):
        for d in range(2):
            receive(d, i)

    for c in norm_z:
        c.wait_recv()
    norm_out[...] = zbuf[:, 0, :]
    for m in range(2):
        for slot in range(nz):
            block = outs[m].at[pl.ds(0, rows)]
            remote(block, block, pair_send, pair_recv.at[m, slot], {"zero": peer}).wait_recv()
    for d in range(2):
        low(d).wait_send()
        for i in range(pieces - DEPTH, pieces):
            ring(d, i).wait_send()
    remote(og, og, pair_send, pair_recv.at[0, 0], {"zero": peer}).wait_send()
    for c in [first, *norm_y, *spread, back, *norm_z]:
        c.wait_send()


def write_out(parts, *refs):
    ins, outs, (scratch, sem) = refs[:4], refs[4:9], refs[9:]
    size = ins[0].shape[0] // parts
    copies = [
        pltpu.make_async_copy(
            ins[m].at[pl.ds(i * size, size)], outs[m].at[pl.ds(i * size, size)], sem.at[m * parts + i]
        )
        for i in range(parts)
        for m in range(2)
    ]
    copies += [pltpu.make_async_copy(ins[2].at[m], outs[2 + m], sem.at[2 * parts + m]) for m in range(2)]
    for c in copies:
        c.start()
    scratch[...] = ins[3][...].astype(jnp.bfloat16)
    last = pltpu.make_async_copy(scratch, outs[4], sem.at[2 * parts + 2])
    last.start()
    for c in copies + [last]:
        c.wait()


def per_device(weight_gate, low_gate, high_gate, weight_up, low_up, high_up, norm_train, norm_step):
    devices, ny = lax.axis_size("zero"), lax.axis_size("cols")
    nz = devices // 2
    rows, columns = weight_gate.shape
    rank = low_gate.shape[1]
    share = norm_train.shape[0]
    tiles = columns // LANES
    f32, bf16 = jnp.float32, jnp.bfloat16
    hbm = pl.BlockSpec(memory_space=pltpu.HBM)
    vmem = pl.BlockSpec(memory_space=pltpu.VMEM)
    dma = pltpu.SemaphoreType.DMA
    serving_gate, serving_up, column, norm = pl.pallas_call(
        functools.partial(kernel, nz, ny),
        out_shape=(
            pltpu.VMEM((devices * rows, columns), bf16),
            pltpu.VMEM((devices * rows, columns), bf16),
            pltpu.VMEM((2, tiles, LANES), f32),
            pltpu.VMEM((devices, LANES), f32),
        ),
        in_specs=[hbm] * 8,
        out_specs=(vmem,) * 4,
        scratch_shapes=[
            pltpu.VMEM((2, rows, columns), bf16),
            pltpu.VMEM((2, rank, rows), bf16),
            pltpu.VMEM((2, rank, columns), bf16),
            pltpu.VMEM((2, 1, share), f32),
            pltpu.VMEM((2, rows, columns), bf16),
            pltpu.VMEM((2, rank, rows), bf16),
            pltpu.VMEM((2, rows, columns), f32),
            pltpu.VMEM((2, tiles, LANES), f32),
            pltpu.VMEM((tiles, LANES), f32),
            pltpu.VMEM((tiles, LANES), f32),
            pltpu.VMEM((nz, tiles, LANES), f32),
            pltpu.VMEM((2, 1, columns), f32),
            pltpu.VMEM((ny, 1, LANES), f32),
            pltpu.VMEM((devices, 1, LANES), f32),
            dma((8,)),
            dma((2, DEPTH)),
            dma((2, (nz - 1) * CH)),
            dma((2,)),
            dma((2,)),
            dma,
            dma((2, nz)),
            dma((nz + 1,)),
            dma((nz + 1,)),
            dma((max(ny - 1, 1),)),
            dma((max(ny - 1, 1),)),
            dma((devices - 1,)),
            dma((devices - 1,)),
        ],
        compiler_params=pltpu.CompilerParams(
            collective_id=0, has_side_effects=True, vmem_limit_bytes=47 << 20
        ),
    )(
        weight_gate, low_gate.T, high_gate, weight_up, low_up.T, high_up,
        norm_train.reshape(1, share), norm_step.reshape(1, share),
    )
    parts = 4
    serving_gate, serving_up, column_gate, column_up, norm = pl.pallas_call(
        functools.partial(write_out, parts),
        out_shape=(
            jax.ShapeDtypeStruct((devices * rows, columns), bf16),
            jax.ShapeDtypeStruct((devices * rows, columns), bf16),
            jax.ShapeDtypeStruct((tiles, LANES), f32),
            jax.ShapeDtypeStruct((tiles, LANES), f32),
            jax.ShapeDtypeStruct((devices, LANES), bf16),
        ),
        in_specs=[vmem] * 4,
        out_specs=(hbm,) * 5,
        scratch_shapes=[pltpu.VMEM((devices, LANES), bf16), dma((2 * parts + 3,))],
        compiler_params=pltpu.CompilerParams(vmem_limit_bytes=20 << 20),
    )(serving_gate, serving_up, column, norm)
    return (serving_gate, serving_up, column_gate.reshape(-1), column_up.reshape(-1), norm.reshape(-1))


def solution(mesh):
    in_specs = (
        P(("job", "zero"), "cols"),
        P(("job", "zero"), None),
        P("job", "cols"),
        P(("job", "zero"), "cols"),
        P(("job", "zero"), None),
        P("job", "cols"),
        P(("job", "zero", "cols")),
        P(("job", "zero", "cols")),
    )
    out_specs = (
        P("job", "cols"),
        P("job", "cols"),
        P(("job", "cols")),
        P(("job", "cols")),
        P("job"),
    )
    return jax.shard_map(
        per_device, mesh=mesh, in_specs=in_specs, out_specs=out_specs, check_vma=False
    )
```

```python
import functools

import jax
import jax.numpy as jnp
from jax import lax
from jax.experimental import pallas as pl
from jax.experimental.pallas import tpu as pltpu
from jax.sharding import PartitionSpec as P

mix_rate = 2.0
MESH = pl.DeviceIdType.MESH
CH = 4
TILE = 512
DEPTH = 8
LAG = 6
EARLY = 3
LANES = 128


def remote(src, dst, send_sem, recv_sem, device_id):
    return pltpu.make_async_remote_copy(
        src_ref=src, dst_ref=dst, send_sem=send_sem, recv_sem=recv_sem, device_id=device_id, device_id_type=MESH
    )


def kernel(
    nz, ny,
    wg_hbm, lg_hbm, hg_hbm, wu_hbm, lu_hbm, hu_hbm, nt_hbm, ns_hbm,
    og, ou, col_out, norm_out,
    w_in, l_in, h_in, n_in, raw, l_raw, whole, pmax, pget, cmax, allmax, inv, ybuf, zbuf,
    in_sem, ring_send, ring_recv, low_send, low_recv, pair_send, pair_recv,
    max_send, max_recv, ny_send, ny_recv, nz_send, nz_recv, known,
):
    zero, col = lax.axis_index("zero"), lax.axis_index("cols")
    z, core = zero // 2, zero % 2
    outs = (og, ou)
    rows, columns = w_in.shape[1:]
    step_rows = rows // CH
    half = nz // 2
    own = 2 * CH
    pieces = (2 * half - 1) * CH

    loads = [
        pltpu.make_async_copy(src, dst, in_sem.at[i])
        for i, (src, dst) in enumerate(
            (
                (wg_hbm, w_in.at[0]), (wu_hbm, w_in.at[1]), (lg_hbm, l_in.at[0]), (lu_hbm, l_in.at[1]),
                (hg_hbm, h_in.at[0]), (hu_hbm, h_in.at[1]), (nt_hbm, n_in.at[0]), (ns_hbm, n_in.at[1]),
            )
        )
    ]
    for c in loads:
        c.start()

    barrier = pltpu.get_barrier_semaphore()
    peer = zero + 1 - 2 * core
    to = ((z + 1) % nz * 2 + core, (z + nz - 1) % nz * 2 + core)
    others = [(z + d) % nz * 2 + core for d in range(1, nz)]
    next_col, last_col = (col + 1) % ny, (col + ny - 1) % ny
    for t in (*to, peer):
        pl.semaphore_signal(barrier, 1, device_id={"zero": t}, device_id_type=MESH)
    for t in (next_col, last_col):
        pl.semaphore_signal(barrier, 1, device_id={"cols": t}, device_id_type=MESH)

    def know(hops):
        pl.semaphore_wait(known.at[hops - 2], 2)

    def tell(hops):
        for t in to:
            pl.semaphore_signal(known.at[hops - 2], 1, device_id={"zero": t}, device_id_type=MESH)

    def merged(weights, low, m, at):
        return weights[:, at].astype(jnp.float32) + mix_rate * lax.dot_general(
            low[...], h_in[m, :, at], (((0,), (0,)), ((), ())), preferred_element_type=jnp.float32
        )

    def maxima(m):
        for t in range(columns // TILE):
            at = slice(t * TILE, (t + 1) * TILE)
            new = merged(w_in.at[m], l_in.at[m], m, at)
            whole[m, :, at] = new
            top = jnp.max(jnp.abs(new), axis=0, keepdims=True)
            for q in range(TILE // LANES):
                r = t * (TILE // LANES) + q
                pmax[m, r : r + 1, :] = top[:, q * LANES : (q + 1) * LANES]

    def block_rows(d, s):
        b = (z - s + nz) % nz if d == 0 else (z + s) % nz
        return (b * 2 + core) * rows

    def matrix(d, k):
        return k // CH if d == 0 else 1 - k // CH

    def piece(d, i, hops):
        k = i % own
        at = pl.multiple_of(block_rows(d, i // own + hops) + k % CH * step_rows, step_rows)
        return outs[matrix(d, k)].at[pl.ds(at, step_rows)]

    def ring(d, i):
        if i < own:
            m, at = matrix(d, i), pl.ds(i % CH * step_rows, step_rows)
            src, dst = w_in.at[m, at], raw.at[d, m, at]
        else:
            src = dst = piece(d, i, 0)
        return remote(src, dst, ring_send.at[d, i % DEPTH], ring_recv.at[d, i], {"zero": to[d]})

    def pair(d, i):
        ref = piece(d, i, 1)
        s = i // own + 1
        slot = s if d == matrix(d, i % own) else (nz - s) % nz
        return remote(ref, ref, pair_send, pair_recv.at[matrix(d, i % own), slot], {"zero": peer})

    def low(d):
        return remote(l_in, l_raw.at[d], low_send.at[d], low_recv.at[d], {"zero": to[d]})

    def norm_y(h):
        row = ybuf.at[(col + ny - h) % ny]
        return remote(row, row, ny_send.at[h], ny_recv.at[h], {"cols": next_col})

    norm_z = [
        remote(zbuf.at[core, z], zbuf.at[core, z], nz_send.at[i], nz_recv.at[i], {"zero": t})
        for i, t in enumerate(others)
    ]
    norm_pair = remote(zbuf.at[core], zbuf.at[core], nz_send.at[nz - 1], nz_recv.at[nz - 1], {"zero": peer})

    for c in loads[:4]:
        c.wait()
    pl.semaphore_wait(barrier, 5)
    tell(2)
    for d in range(2):
        ring(d, 0).start()
    for d in range(2):
        low(d).start()
        for i in range(1, EARLY):
            ring(d, i).start()
    for c in loads[4:]:
        c.wait()
    gain = n_in[0] + n_in[1]
    ybuf[pl.ds(col, 1)] = jnp.concatenate([gain] * ny, axis=1)[None]
    maxima(0)
    know(2)
    tell(3)
    maxima(1)
    know(3)
    tell(4)

    first = remote(pmax.at[1 - core], pget, max_send.at[0], max_recv.at[0], {"zero": peer})
    first.start()
    norm_y(0).start()
    first.wait_recv()
    cmax[...] = jnp.maximum(pmax[core], pget[...])
    know(4)
    spread = [
        remote(cmax, allmax.at[d], max_send.at[d], max_recv.at[d], {"zero": others[d - 1]}) for d in range(1, nz)
    ]
    for c in spread:
        c.start()
    for i in range(EARLY, own):
        for d in range(2):
            ring(d, i).start()
    for h in range(1, ny - 1):
        norm_y(h - 1).wait_recv()
        norm_y(h).start()
    top = cmax[...]
    for d, c in enumerate(spread):
        c.wait_recv()
        top = jnp.maximum(top, allmax[d + 1])
    col_out[pl.ds(core, 1)] = top[None]
    back = remote(col_out.at[core], col_out.at[core], max_send.at[nz], max_recv.at[nz], {"zero": peer})
    back.start()
    norm_y(ny - 2).wait_recv()
    lane = lax.broadcasted_iota(jnp.int32, (1, LANES), 1) // (LANES // ny)
    row = ybuf[0]
    for k in range(1, ny):
        row = jnp.where(lane == k, ybuf[k], row)
    zbuf[pl.ds(core, 1), pl.ds(z, 1)] = row[None, None]
    back.wait_recv()
    for m in range(2):
        for r in range(columns // LANES):
            inv[m, :, r * LANES : (r + 1) * LANES] = 1.0 / col_out[m, r : r + 1, :]

    def near(d, m):
        first_row = pl.multiple_of(block_rows(d, 1), rows)
        for t in range(columns // TILE):
            at = slice(t * TILE, (t + 1) * TILE)
            new = merged(raw.at[d, m], l_raw.at[d, m], m, at) * inv[m, :, at]
            outs[m][pl.ds(first_row, rows), at] = new.astype(jnp.bfloat16)

    def near_half(h):
        for d in range(2):
            if h == 0:
                low(d).wait_recv()
            for k in range(h * CH, (h + 1) * CH):
                ring(d, k).wait_recv()
            near(d, matrix(d, h * CH))

    mine = pl.multiple_of(zero * rows, rows)
    sent = [0, 0]

    def drain(d, i):
        while sent[d] <= i:
            ring(d, sent[d]).wait_send()
            sent[d] += 1

    def receive(d, i):
        ring(d, i).wait_recv()
        pair(d, i).start()

    for i in range(own, pieces):
        if i == own:
            near_half(0)
        if i == own + CH:
            near_half(1)
        for d in range(2):
            drain(d, i - DEPTH)
            ring(d, i).start()
            if i < 2 * own:
                pair(d, i - own).start()
        if i == own + 1:
            for c in norm_z:
                c.start()
            for m in range(2):
                for t in range(columns // TILE):
                    at = slice(t * TILE, (t + 1) * TILE)
                    outs[m][pl.ds(mine, rows), at] = (whole[m, :, at] * inv[m, :, at]).astype(jnp.bfloat16)
        if i == own + 2:
            for m in range(2):
                block = outs[m].at[pl.ds(mine, rows)]
                remote(block, block, pair_send, pair_recv.at[m, 0], {"zero": peer}).start()
        if i == 2 * own:
            for c in norm_z:
                c.wait_recv()
            norm_pair.start()
        if i - LAG >= own:
            for d in range(2):
                receive(d, i - LAG)
    for i in range(pieces - LAG, pieces):
        for d in range(2):
            receive(d, i)

    norm_pair.wait_recv()
    for k in range(nz):
        for c in range(2):
            norm_out[2 * k + c : 2 * k + c + 1, :] = zbuf[c, k]
    for d in range(2):
        low(d).wait_send()
        drain(d, pieces - 1)
    for c in [first, *spread, back, *norm_z, norm_pair]:
        c.wait_send()
    for h in range(ny - 1):
        norm_y(h).wait_send()
    for m in range(2):
        for slot in range(nz):
            block = outs[m].at[pl.ds(0, rows)]
            remote(block, block, pair_send, pair_recv.at[m, slot], {"zero": peer}).wait_recv()
    remote(og, og, pair_send, pair_recv.at[0, 0], {"zero": peer}).wait_send()


def write_out(parts, *refs):
    ins, outs, (scratch, sem) = refs[:4], refs[4:9], refs[9:]
    size = ins[0].shape[0] // parts
    copies = [
        pltpu.make_async_copy(
            ins[m].at[pl.ds(i * size, size)], outs[m].at[pl.ds(i * size, size)], sem.at[m * parts + i]
        )
        for i in range(parts)
        for m in range(2)
    ]
    copies += [pltpu.make_async_copy(ins[2].at[m], outs[2 + m], sem.at[2 * parts + m]) for m in range(2)]
    for c in copies:
        c.start()
    scratch[...] = ins[3][...].astype(jnp.bfloat16)
    last = pltpu.make_async_copy(scratch, outs[4], sem.at[2 * parts + 2])
    last.start()
    for c in copies + [last]:
        c.wait()


def per_device(weight_gate, low_gate, high_gate, weight_up, low_up, high_up, norm_train, norm_step):
    devices, ny = lax.axis_size("zero"), lax.axis_size("cols")
    nz = devices // 2
    rows, columns = weight_gate.shape
    rank = low_gate.shape[1]
    share = norm_train.shape[0]
    tiles = columns // LANES
    f32, bf16 = jnp.float32, jnp.bfloat16
    hbm = pl.BlockSpec(memory_space=pltpu.HBM)
    vmem = pl.BlockSpec(memory_space=pltpu.VMEM)
    dma = pltpu.SemaphoreType.DMA
    serving_gate, serving_up, column, norm = pl.pallas_call(
        functools.partial(kernel, nz, ny),
        out_shape=(
            pltpu.VMEM((devices * rows, columns), bf16),
            pltpu.VMEM((devices * rows, columns), bf16),
            pltpu.VMEM((2, tiles, LANES), f32),
            pltpu.VMEM((devices, LANES), f32),
        ),
        in_specs=[hbm] * 8,
        out_specs=(vmem,) * 4,
        scratch_shapes=[
            pltpu.VMEM((2, rows, columns), bf16),
            pltpu.VMEM((2, rank, rows), bf16),
            pltpu.VMEM((2, rank, columns), bf16),
            pltpu.VMEM((2, 1, share), f32),
            pltpu.VMEM((2, 2, rows, columns), bf16),
            pltpu.VMEM((2, 2, rank, rows), bf16),
            pltpu.VMEM((2, rows, columns), f32),
            pltpu.VMEM((2, tiles, LANES), f32),
            pltpu.VMEM((tiles, LANES), f32),
            pltpu.VMEM((tiles, LANES), f32),
            pltpu.VMEM((nz, tiles, LANES), f32),
            pltpu.VMEM((2, 1, columns), f32),
            pltpu.VMEM((ny, 1, LANES), f32),
            pltpu.VMEM((2, nz, 1, LANES), f32),
            dma((8,)),
            dma((2, DEPTH)),
            dma((2, (nz - 1) * CH)),
            dma((2,)),
            dma((2,)),
            dma,
            dma((2, nz)),
            dma((nz + 1,)),
            dma((nz + 1,)),
            dma((ny - 1,)),
            dma((ny - 1,)),
            dma((nz,)),
            dma((nz,)),
            pltpu.SemaphoreType.REGULAR((3,)),
        ],
        compiler_params=pltpu.CompilerParams(
            collective_id=0, has_side_effects=True, vmem_limit_bytes=47 << 20
        ),
    )(
        weight_gate, low_gate.T, high_gate, weight_up, low_up.T, high_up,
        norm_train.reshape(1, share), norm_step.reshape(1, share),
    )
    parts = 4
    serving_gate, serving_up, column_gate, column_up, norm = pl.pallas_call(
        functools.partial(write_out, parts),
        out_shape=(
            jax.ShapeDtypeStruct((devices * rows, columns), bf16),
            jax.ShapeDtypeStruct((devices * rows, columns), bf16),
            jax.ShapeDtypeStruct((tiles, LANES), f32),
            jax.ShapeDtypeStruct((tiles, LANES), f32),
            jax.ShapeDtypeStruct((devices, LANES), bf16),
        ),
        in_specs=[vmem] * 4,
        out_specs=(hbm,) * 5,
        scratch_shapes=[pltpu.VMEM((devices, LANES), bf16), dma((2 * parts + 3,))],
        compiler_params=pltpu.CompilerParams(vmem_limit_bytes=20 << 20),
    )(serving_gate, serving_up, column, norm)
    return (serving_gate, serving_up, column_gate.reshape(-1), column_up.reshape(-1), norm.reshape(-1))


def solution(mesh):
    in_specs = (
        P(("job", "zero"), "cols"),
        P(("job", "zero"), None),
        P("job", "cols"),
        P(("job", "zero"), "cols"),
        P(("job", "zero"), None),
        P("job", "cols"),
        P(("job", "zero", "cols")),
        P(("job", "zero", "cols")),
    )
    out_specs = (
        P("job", "cols"),
        P("job", "cols"),
        P(("job", "cols")),
        P(("job", "cols")),
        P("job"),
    )
    return jax.shard_map(
        per_device, mesh=mesh, in_specs=in_specs, out_specs=out_specs, check_vma=False
    )
```

```python
import functools

import jax
import jax.numpy as jnp
from jax import lax
from jax.experimental import pallas as pl
from jax.experimental.pallas import tpu as pltpu
from jax.sharding import PartitionSpec as P

mix_rate = 2.0
MESH = pl.DeviceIdType.MESH
CH = 4
TILE = 512
DEPTH = 8
LAG = 6
EARLY = (4, 2)
LANES = 128


def remote(src, dst, send_sem, recv_sem, device_id):
    return pltpu.make_async_remote_copy(
        src_ref=src, dst_ref=dst, send_sem=send_sem, recv_sem=recv_sem, device_id=device_id, device_id_type=MESH
    )


def kernel(
    nz, ny,
    wg_hbm, lg_hbm, hg_hbm, wu_hbm, lu_hbm, hu_hbm, nt_hbm, ns_hbm,
    og, ou, col_out, norm_out,
    w_in, l_in, h_in, n_in, raw, l_raw, whole, pmax, pget, cmax, allmax, inv, ybuf, zbuf,
    in_sem, ring_send, ring_recv, rest_send, rest_recv, low_send, low_recv, pair_send, pair_recv,
    max_send, max_recv, ny_send, ny_recv, nz_send, nz_recv, known,
):
    zero, col = lax.axis_index("zero"), lax.axis_index("cols")
    z, core = zero // 2, zero % 2
    outs = (og, ou)
    rows, columns = w_in.shape[1:]
    step_rows = rows // CH
    half = nz // 2
    own = 2 * CH
    pieces = (2 * half - 1) * CH

    loads = [
        pltpu.make_async_copy(src, dst, in_sem.at[i])
        for i, (src, dst) in enumerate(
            (
                (wg_hbm, w_in.at[0]), (wu_hbm, w_in.at[1]), (lg_hbm, l_in.at[0]), (lu_hbm, l_in.at[1]),
                (hg_hbm, h_in.at[0]), (hu_hbm, h_in.at[1]), (nt_hbm, n_in.at[0]), (ns_hbm, n_in.at[1]),
            )
        )
    ]
    for c in loads:
        c.start()

    barrier = pltpu.get_barrier_semaphore()
    peer = zero + 1 - 2 * core
    to = ((z + 1) % nz * 2 + core, (z + nz - 1) % nz * 2 + core)
    others = [(z + d) % nz * 2 + core for d in range(1, nz)]
    for t in (*to, peer):
        pl.semaphore_signal(barrier, 1, device_id={"zero": t}, device_id_type=MESH)
    sides = (col + 1 < ny, col > 0)
    beside = (lax.rem(col + 1, ny), lax.rem(col + ny - 1, ny))
    for e in range(2):

        @pl.when(sides[e])
        def _():
            pl.semaphore_signal(barrier, 1, device_id={"cols": beside[e]}, device_id_type=MESH)


    def know(hops):
        pl.semaphore_wait(known.at[hops - 2], 2)

    def tell(hops):
        for t in to:
            pl.semaphore_signal(known.at[hops - 2], 1, device_id={"zero": t}, device_id_type=MESH)

    def merged(weights, low, m, at):
        return weights[:, at].astype(jnp.float32) + mix_rate * lax.dot_general(
            low[...], h_in[m, :, at], (((0,), (0,)), ((), ())), preferred_element_type=jnp.float32
        )

    def maxima(m):
        for t in range(columns // TILE):
            at = slice(t * TILE, (t + 1) * TILE)
            new = merged(w_in.at[m], l_in.at[m], m, at)
            whole[m, :, at] = new
            top = jnp.max(jnp.abs(new), axis=0, keepdims=True)
            for q in range(TILE // LANES):
                r = t * (TILE // LANES) + q
                pmax[m, r : r + 1, :] = top[:, q * LANES : (q + 1) * LANES]

    def block_rows(d, s):
        b = (z - s + nz) % nz if d == 0 else (z + s) % nz
        return (b * 2 + core) * rows

    def matrix(d, k):
        return k // CH if d == 0 else 1 - k // CH

    def chunk(k):
        return k * step_rows if k < CH else (own - 1 - k) * step_rows

    split = step_rows // 2

    def piece(d, i, hops):
        size = step_rows - split if (d, i) == (0, pieces - 1) else step_rows
        at = pl.multiple_of(block_rows(d, i // own + hops) + chunk(i % own), split)
        return outs[matrix(d, i % own)].at[pl.ds(at, size)]

    def rest(d, hops):
        at = pl.multiple_of(block_rows(d, half - 1 + hops) + chunk(CH - 1) + step_rows - split, split)
        return og.at[pl.ds(at, split)]

    def rest_ring(d):
        ref = rest(d, 0)
        return remote(ref, ref, rest_send.at[d], rest_recv.at[d], {"zero": to[d]})

    def rest_pair(d):
        ref = rest(d, 1)
        return remote(ref, ref, pair_send, pair_recv.at[0, half], {"zero": peer})

    def ring(d, i):
        if i < own:
            m, at = matrix(d, i), pl.ds(chunk(i), step_rows)
            src, dst = w_in.at[m, at], raw.at[d, m, at]
        else:
            src = dst = piece(d, i, 0)
        return remote(src, dst, ring_send.at[d, i % DEPTH], ring_recv.at[d, i], {"zero": to[d]})

    def pair(d, i):
        ref = piece(d, i, 1)
        s = i // own + 1
        slot = s if d == matrix(d, i % own) else (nz - s) % nz
        return remote(ref, ref, pair_send, pair_recv.at[matrix(d, i % own), slot], {"zero": peer})

    def low(d):
        return remote(l_in, l_raw.at[d], low_send.at[d], low_recv.at[d], {"zero": to[d]})

    def norm_y(e, h):
        row = ybuf.at[lax.rem(col + ny - h, ny) if e == 0 else lax.rem(col + h, ny)]
        return remote(row, row, ny_send.at[e, h], ny_recv.at[e, h], {"cols": beside[e]})

    def gives(e, h):
        return (sides[0] & (col >= h), sides[1] & (col + h < ny))[e]

    def gets(e, h):
        return (col >= h + 1, col + h + 1 < ny)[e]

    def norm_y_start(h):
        for e in range(2):

            @pl.when(gives(e, h))
            def _():
                norm_y(e, h).start()

    def norm_y_get(h):
        for e in range(2):

            @pl.when(gets(e, h))
            def _():
                norm_y(e, h).wait_recv()

    norm_z = [
        remote(zbuf.at[core, z], zbuf.at[core, z], nz_send.at[i], nz_recv.at[i], {"zero": t})
        for i, t in enumerate(others)
    ]
    norm_pair = remote(zbuf.at[core], zbuf.at[core], nz_send.at[nz - 1], nz_recv.at[nz - 1], {"zero": peer})

    for c in loads[:4]:
        c.wait()
    pl.semaphore_wait(barrier, 3 + sides[0].astype(jnp.int32) + sides[1].astype(jnp.int32))
    tell(2)
    for d in range(2):
        ring(d, 0).start()
    for d in range(2):
        low(d).start()
        for i in range(1, EARLY[1]):
            ring(d, i).start()

    def between():
        for i in range(EARLY[1], EARLY[0]):
            for d in range(2):
                ring(d, i).start()

    pl.when(z < half)(between)
    for c in loads[4:]:
        c.wait()
    gain = n_in[0] + n_in[1]
    ybuf[pl.ds(col, 1)] = jnp.concatenate([gain] * ny, axis=1)[None]
    maxima(0)
    know(2)
    tell(3)
    maxima(1)
    know(3)
    tell(4)

    first = remote(pmax.at[1 - core], pget, max_send.at[0], max_recv.at[0], {"zero": peer})
    first.start()
    norm_y_start(0)
    first.wait_recv()
    cmax[...] = jnp.maximum(pmax[core], pget[...])
    know(4)
    spread = [
        remote(cmax, allmax.at[d], max_send.at[d], max_recv.at[d], {"zero": others[d - 1]}) for d in range(1, nz)
    ]
    for c in spread:
        c.start()
    pl.when(z >= half)(between)
    for i in range(EARLY[0], own):
        for d in range(2):
            ring(d, i).start()
    for h in range(1, ny - 1):
        norm_y_get(h - 1)
        norm_y_start(h)
    top = cmax[...]
    for d, c in enumerate(spread):
        c.wait_recv()
        top = jnp.maximum(top, allmax[d + 1])
    col_out[pl.ds(core, 1)] = top[None]
    back = remote(col_out.at[core], col_out.at[core], max_send.at[nz], max_recv.at[nz], {"zero": peer})
    back.start()
    norm_y_get(ny - 2)
    lane = lax.broadcasted_iota(jnp.int32, (1, LANES), 1) // (LANES // ny)
    row = ybuf[0]
    for k in range(1, ny):
        row = jnp.where(lane == k, ybuf[k], row)
    zbuf[pl.ds(core, 1), pl.ds(z, 1)] = row[None, None]
    back.wait_recv()
    for m in range(2):
        for r in range(columns // LANES):
            inv[m, :, r * LANES : (r + 1) * LANES] = 1.0 / col_out[m, r : r + 1, :]

    def near(d, m):
        first_row = pl.multiple_of(block_rows(d, 1), rows)
        for t in range(columns // TILE):
            at = slice(t * TILE, (t + 1) * TILE)
            new = merged(raw.at[d, m], l_raw.at[d, m], m, at) * inv[m, :, at]
            outs[m][pl.ds(first_row, rows), at] = new.astype(jnp.bfloat16)

    def near_half(h):
        for d in range(2):
            if h == 0:
                low(d).wait_recv()
            for k in range(h * CH, (h + 1) * CH):
                ring(d, k).wait_recv()
            near(d, matrix(d, h * CH))

    mine = pl.multiple_of(zero * rows, rows)
    sent = [0, 0]

    def drain(d, i):
        while sent[d] <= i:
            ring(d, sent[d]).wait_send()
            sent[d] += 1

    def receive(d, i):
        ring(d, i).wait_recv()
        pair(d, i).start()

    for i in range(own, pieces):
        if i == own:
            near_half(0)
        if i == own + CH:
            near_half(1)
        for d in range(2):
            drain(d, i - DEPTH)
            ring(d, i).start()
            if i < 2 * own:
                pair(d, i - own).start()
        if i == own + 1:
            for c in norm_z:
                c.start()
            for m in range(2):
                for t in range(columns // TILE):
                    at = slice(t * TILE, (t + 1) * TILE)
                    outs[m][pl.ds(mine, rows), at] = (whole[m, :, at] * inv[m, :, at]).astype(jnp.bfloat16)
        if i == own + 2:
            for m in range(2):
                block = outs[m].at[pl.ds(mine, rows)]
                remote(block, block, pair_send, pair_recv.at[m, 0], {"zero": peer}).start()
        if i == 2 * own:
            for c in norm_z:
                c.wait_recv()
            norm_pair.start()
        if i - LAG >= own:
            for d in range(2):
                receive(d, i - LAG)
    pl.when(z != nz - 1)(lambda: rest_ring(0).start())
    pl.when(z == 1)(lambda: rest_ring(1).start())
    for i in range(pieces - LAG, pieces):
        for d in range(2):
            receive(d, i)
    for d, here in ((0, z != 0), (1, z == 0)):

        @pl.when(here)
        def _():
            rest_ring(d).wait_recv()
            rest_pair(d).start()


    norm_pair.wait_recv()
    for k in range(nz):
        for c in range(2):
            norm_out[2 * k + c : 2 * k + c + 1, :] = zbuf[c, k]
    for d in range(2):
        low(d).wait_send()
        drain(d, pieces - 1)
    for c in [first, *spread, back, *norm_z, norm_pair]:
        c.wait_send()
    for h in range(ny - 1):
        for e in range(2):

            @pl.when(gives(e, h))
            def _():
                norm_y(e, h).wait_send()

    pl.when(z != nz - 1)(lambda: rest_ring(0).wait_send())
    pl.when(z == 1)(lambda: rest_ring(1).wait_send())
    for m in range(2):
        for slot in range(nz):
            block = outs[m].at[pl.ds(0, rows)]
            remote(block, block, pair_send, pair_recv.at[m, slot], {"zero": peer}).wait_recv()
    remote(og, og, pair_send, pair_recv.at[0, 0], {"zero": peer}).wait_send()


def write_out(parts, *refs):
    ins, outs, (scratch, sem) = refs[:4], refs[4:9], refs[9:]
    size = ins[0].shape[0] // parts
    copies = [
        pltpu.make_async_copy(
            ins[m].at[pl.ds(i * size, size)], outs[m].at[pl.ds(i * size, size)], sem.at[m * parts + i]
        )
        for i in range(parts)
        for m in range(2)
    ]
    copies += [pltpu.make_async_copy(ins[2].at[m], outs[2 + m], sem.at[2 * parts + m]) for m in range(2)]
    for c in copies:
        c.start()
    scratch[...] = ins[3][...].astype(jnp.bfloat16)
    last = pltpu.make_async_copy(scratch, outs[4], sem.at[2 * parts + 2])
    last.start()
    for c in copies + [last]:
        c.wait()


def per_device(weight_gate, low_gate, high_gate, weight_up, low_up, high_up, norm_train, norm_step):
    devices, ny = lax.axis_size("zero"), lax.axis_size("cols")
    nz = devices // 2
    rows, columns = weight_gate.shape
    rank = low_gate.shape[1]
    share = norm_train.shape[0]
    tiles = columns // LANES
    f32, bf16 = jnp.float32, jnp.bfloat16
    hbm = pl.BlockSpec(memory_space=pltpu.HBM)
    vmem = pl.BlockSpec(memory_space=pltpu.VMEM)
    dma = pltpu.SemaphoreType.DMA
    serving_gate, serving_up, column, norm = pl.pallas_call(
        functools.partial(kernel, nz, ny),
        out_shape=(
            pltpu.VMEM((devices * rows, columns), bf16),
            pltpu.VMEM((devices * rows, columns), bf16),
            pltpu.VMEM((2, tiles, LANES), f32),
            pltpu.VMEM((devices, LANES), f32),
        ),
        in_specs=[hbm] * 8,
        out_specs=(vmem,) * 4,
        scratch_shapes=[
            pltpu.VMEM((2, rows, columns), bf16),
            pltpu.VMEM((2, rank, rows), bf16),
            pltpu.VMEM((2, rank, columns), bf16),
            pltpu.VMEM((2, 1, share), f32),
            pltpu.VMEM((2, 2, rows, columns), bf16),
            pltpu.VMEM((2, 2, rank, rows), bf16),
            pltpu.VMEM((2, rows, columns), f32),
            pltpu.VMEM((2, tiles, LANES), f32),
            pltpu.VMEM((tiles, LANES), f32),
            pltpu.VMEM((tiles, LANES), f32),
            pltpu.VMEM((nz, tiles, LANES), f32),
            pltpu.VMEM((2, 1, columns), f32),
            pltpu.VMEM((ny, 1, LANES), f32),
            pltpu.VMEM((2, nz, 1, LANES), f32),
            dma((8,)),
            dma((2, DEPTH)),
            dma((2, (nz - 1) * CH)),
            dma((2,)),
            dma((2,)),
            dma((2,)),
            dma((2,)),
            dma,
            dma((2, nz)),
            dma((nz + 1,)),
            dma((nz + 1,)),
            dma((2, ny - 1)),
            dma((2, ny - 1)),
            dma((nz,)),
            dma((nz,)),
            pltpu.SemaphoreType.REGULAR((3,)),
        ],
        compiler_params=pltpu.CompilerParams(
            collective_id=0, has_side_effects=True, vmem_limit_bytes=47 << 20
        ),
    )(
        weight_gate, low_gate.T, high_gate, weight_up, low_up.T, high_up,
        norm_train.reshape(1, share), norm_step.reshape(1, share),
    )
    parts = 4
    serving_gate, serving_up, column_gate, column_up, norm = pl.pallas_call(
        functools.partial(write_out, parts),
        out_shape=(
            jax.ShapeDtypeStruct((devices * rows, columns), bf16),
            jax.ShapeDtypeStruct((devices * rows, columns), bf16),
            jax.ShapeDtypeStruct((tiles, LANES), f32),
            jax.ShapeDtypeStruct((tiles, LANES), f32),
            jax.ShapeDtypeStruct((devices, LANES), bf16),
        ),
        in_specs=[vmem] * 4,
        out_specs=(hbm,) * 5,
        scratch_shapes=[pltpu.VMEM((devices, LANES), bf16), dma((2 * parts + 3,))],
        compiler_params=pltpu.CompilerParams(vmem_limit_bytes=20 << 20),
    )(serving_gate, serving_up, column, norm)
    return (serving_gate, serving_up, column_gate.reshape(-1), column_up.reshape(-1), norm.reshape(-1))


def solution(mesh):
    in_specs = (
        P(("job", "zero"), "cols"),
        P(("job", "zero"), None),
        P("job", "cols"),
        P(("job", "zero"), "cols"),
        P(("job", "zero"), None),
        P("job", "cols"),
        P(("job", "zero", "cols")),
        P(("job", "zero", "cols")),
    )
    out_specs = (
        P("job", "cols"),
        P("job", "cols"),
        P(("job", "cols")),
        P(("job", "cols")),
        P("job"),
    )
    return jax.shard_map(
        per_device, mesh=mesh, in_specs=in_specs, out_specs=out_specs, check_vma=False
    )
```

```python
import functools

import jax
import jax.numpy as jnp
from jax import lax
from jax.experimental import pallas as pl
from jax.experimental.pallas import tpu as pltpu
from jax.sharding import PartitionSpec as P

mix_rate = 2.0
MESH = pl.DeviceIdType.MESH
CH = 4
TILE = 512
DEPTH = 8
LAG = 6
EARLY = (4, 3)
LANES = 128


def remote(src, dst, send_sem, recv_sem, device_id):
    return pltpu.make_async_remote_copy(
        src_ref=src, dst_ref=dst, send_sem=send_sem, recv_sem=recv_sem, device_id=device_id, device_id_type=MESH
    )


def kernel(
    nz, ny,
    wg_hbm, lg_hbm, hg_hbm, wu_hbm, lu_hbm, hu_hbm, nt_hbm, ns_hbm,
    og, ou, col_out, norm_out,
    w_in, l_in, h_in, n_in, raw, l_raw, whole, pmax, pget, cmax, allmax, inv, ybuf, zbuf,
    in_sem, ring_send, ring_recv, rest_send, rest_recv, low_send, low_recv, pair_send, pair_recv,
    max_send, max_recv, ny_send, ny_recv, nz_send, nz_recv, known, answer,
):
    zero, col = lax.axis_index("zero"), lax.axis_index("cols")
    z, core = zero // 2, zero % 2
    outs = (og, ou)
    rows, columns = w_in.shape[1:]
    step_rows = rows // CH
    half = nz // 2
    own = 2 * CH
    pieces = (2 * half - 1) * CH

    loads = [
        pltpu.make_async_copy(src, dst, in_sem.at[i])
        for i, (src, dst) in enumerate(
            (
                (wg_hbm, w_in.at[0]), (wu_hbm, w_in.at[1]), (lg_hbm, l_in.at[0]), (lu_hbm, l_in.at[1]),
                (hg_hbm, h_in.at[0]), (hu_hbm, h_in.at[1]), (nt_hbm, n_in.at[0]), (ns_hbm, n_in.at[1]),
            )
        )
    ]
    for c in loads:
        c.start()

    barrier = pltpu.get_barrier_semaphore()
    peer = zero + 1 - 2 * core
    to = ((z + 1) % nz * 2 + core, (z + nz - 1) % nz * 2 + core)
    others = [(z + d) % nz * 2 + core for d in range(1, nz)]
    sides = (col + 1 < ny, col > 0)
    beside = (lax.rem(col + 1, ny), lax.rem(col + ny - 1, ny))

    def signal(sem, axis, index):
        pl.semaphore_signal(sem, 1, device_id={axis: index}, device_id_type=MESH)

    low_end, high_end = z == 0, z == nz - 1
    pl.when(z < nz - 2)(lambda: signal(barrier, "zero", to[0]))
    pl.when(low_end | high_end)(lambda: signal(barrier, "zero", to[1]))
    pl.when(core == 1)(lambda: signal(barrier, "zero", peer))
    pl.when(sides[0])(lambda: signal(barrier, "cols", beside[0]))

    def greeted():
        count = sum(c.astype(jnp.int32) for c in (z > 0, z == nz - 2, core == 0, sides[1]))
        pl.when(count > 0)(lambda: pl.semaphore_wait(barrier, count))
        pl.when((z > 0) & (z < nz - 1))(lambda: signal(answer.at[0], "zero", to[1]))
        pl.when(z >= nz - 2)(lambda: signal(answer.at[1], "zero", to[0]))
        pl.when(core == 0)(lambda: signal(answer.at[2], "zero", peer))
        pl.when(sides[1])(lambda: signal(answer.at[3], "cols", beside[1]))

    def know(hops):
        pl.semaphore_wait(known.at[hops - 2], 2)

    def tell(hops):
        for t in to:
            pl.semaphore_signal(known.at[hops - 2], 1, device_id={"zero": t}, device_id_type=MESH)

    def merged(weights, low, m, at):
        return weights[:, at].astype(jnp.float32) + mix_rate * lax.dot_general(
            low[...], h_in[m, :, at], (((0,), (0,)), ((), ())), preferred_element_type=jnp.float32
        )

    def maxima(m):
        for t in range(columns // TILE):
            at = slice(t * TILE, (t + 1) * TILE)
            new = merged(w_in.at[m], l_in.at[m], m, at)
            whole[m, :, at] = new
            top = jnp.max(jnp.abs(new), axis=0, keepdims=True)
            for q in range(TILE // LANES):
                r = t * (TILE // LANES) + q
                pmax[m, r : r + 1, :] = top[:, q * LANES : (q + 1) * LANES]

    def block_rows(d, s):
        b = (z - s + nz) % nz if d == 0 else (z + s) % nz
        return (b * 2 + core) * rows

    def matrix(d, k):
        return k // CH if d == 0 else 1 - k // CH

    def chunk(k):
        return k * step_rows if k < CH else (own - 1 - k) * step_rows

    split = step_rows // 2

    def piece(d, i, hops):
        size = step_rows - split if (d, i) == (0, pieces - 1) else step_rows
        at = pl.multiple_of(block_rows(d, i // own + hops) + chunk(i % own), split)
        return outs[matrix(d, i % own)].at[pl.ds(at, size)]

    def rest(d, hops):
        at = pl.multiple_of(block_rows(d, half - 1 + hops) + chunk(CH - 1) + step_rows - split, split)
        return og.at[pl.ds(at, split)]

    def rest_ring(d):
        ref = rest(d, 0)
        return remote(ref, ref, rest_send.at[d], rest_recv.at[d], {"zero": to[d]})

    def rest_pair(d):
        ref = rest(d, 1)
        return remote(ref, ref, pair_send, pair_recv.at[0, half], {"zero": peer})

    def ring(d, i):
        if i < own:
            m, at = matrix(d, i), pl.ds(chunk(i), step_rows)
            src = (wg_hbm, wu_hbm)[m].at[at] if i < EARLY[1] else w_in.at[m, at]
            dst = raw.at[d, m, at]
        else:
            src = dst = piece(d, i, 0)
        return remote(src, dst, ring_send.at[d, i % DEPTH], ring_recv.at[d, i], {"zero": to[d]})

    def pair(d, i):
        ref = piece(d, i, 1)
        s = i // own + 1
        slot = s if d == matrix(d, i % own) else (nz - s) % nz
        return remote(ref, ref, pair_send, pair_recv.at[matrix(d, i % own), slot], {"zero": peer})

    def low(d):
        return remote(l_in, l_raw.at[d], low_send.at[d], low_recv.at[d], {"zero": to[d]})

    def norm_y(e, h):
        row = ybuf.at[lax.rem(col + ny - h, ny) if e == 0 else lax.rem(col + h, ny)]
        return remote(row, row, ny_send.at[e, h], ny_recv.at[e, h], {"cols": beside[e]})

    def gives(e, h):
        return (sides[0] & (col >= h), sides[1] & (col + h < ny))[e]

    def gets(e, h):
        return (col >= h + 1, col + h + 1 < ny)[e]

    def norm_y_start(h):
        for e in range(2):

            @pl.when(gives(e, h))
            def _():
                norm_y(e, h).start()

    def norm_y_get(h):
        for e in range(2):

            @pl.when(gets(e, h))
            def _():
                norm_y(e, h).wait_recv()

    norm_z = [
        remote(zbuf.at[core, z], zbuf.at[core, z], nz_send.at[i], nz_recv.at[i], {"zero": t})
        for i, t in enumerate(others)
    ]
    norm_pair = remote(zbuf.at[core], zbuf.at[core], nz_send.at[nz - 1], nz_recv.at[nz - 1], {"zero": peer})

    greeted()

    def begin(d):
        for i in range(EARLY[1]):
            ring(d, i).start()

    def between():
        for i in range(EARLY[1], EARLY[0]):
            for d in range(2):
                ring(d, i).start()

    pl.when((z > 0) & (z < nz - 1))(lambda: begin(1))
    pl.when(z < nz - 2)(lambda: pl.semaphore_wait(answer.at[0], 1))
    begin(0)

    @pl.when(high_end)
    def _():
        pl.semaphore_wait(answer.at[1], 1)
        begin(1)

    pl.when(z > 0)(lambda: tell(2))
    for c in loads:
        c.wait()
    pl.when((z > 0) & (z < half))(between)
    gain = n_in[0] + n_in[1]
    ybuf[pl.ds(col, 1)] = jnp.concatenate([gain] * ny, axis=1)[None]
    maxima(0)

    @pl.when(low_end)
    def _():
        for i in range(EARLY[1], EARLY[0]):
            ring(0, i).start()
        pl.semaphore_wait(answer.at[1], 1)
        tell(2)
        begin(1)
        for i in range(EARLY[1], EARLY[0]):
            ring(1, i).start()

    for d in range(2):
        low(d).start()
    maxima(1)
    know(2)
    tell(3)
    pl.when(core == 1)(lambda: pl.semaphore_wait(answer.at[2], 1))
    pl.when(sides[0])(lambda: pl.semaphore_wait(answer.at[3], 1))

    first = remote(pmax.at[1 - core], pget, max_send.at[0], max_recv.at[0], {"zero": peer})
    first.start()
    norm_y_start(0)
    know(3)
    tell(4)
    first.wait_recv()
    cmax[...] = jnp.maximum(pmax[core], pget[...])
    know(4)
    spread = [
        remote(cmax, allmax.at[d], max_send.at[d], max_recv.at[d], {"zero": others[d - 1]}) for d in range(1, nz)
    ]
    for c in spread:
        c.start()
    pl.when(z >= half)(between)
    for i in range(EARLY[0], own):
        for d in range(2):
            ring(d, i).start()
    for h in range(1, ny - 1):
        norm_y_get(h - 1)
        norm_y_start(h)
    top = cmax[...]
    for d, c in enumerate(spread):
        c.wait_recv()
        top = jnp.maximum(top, allmax[d + 1])
    col_out[pl.ds(core, 1)] = top[None]
    back = remote(col_out.at[core], col_out.at[core], max_send.at[nz], max_recv.at[nz], {"zero": peer})
    back.start()
    norm_y_get(ny - 2)
    lane = lax.broadcasted_iota(jnp.int32, (1, LANES), 1) // (LANES // ny)
    row = ybuf[0]
    for k in range(1, ny):
        row = jnp.where(lane == k, ybuf[k], row)
    zbuf[pl.ds(core, 1), pl.ds(z, 1)] = row[None, None]
    back.wait_recv()
    for m in range(2):
        for r in range(columns // LANES):
            inv[m, :, r * LANES : (r + 1) * LANES] = 1.0 / col_out[m, r : r + 1, :]

    def near(d, m):
        first_row = pl.multiple_of(block_rows(d, 1), rows)
        for t in range(columns // TILE):
            at = slice(t * TILE, (t + 1) * TILE)
            new = merged(raw.at[d, m], l_raw.at[d, m], m, at) * inv[m, :, at]
            outs[m][pl.ds(first_row, rows), at] = new.astype(jnp.bfloat16)

    def near_half(h):
        for d in range(2):
            if h == 0:
                low(d).wait_recv()
            for k in range(h * CH, (h + 1) * CH):
                ring(d, k).wait_recv()
            near(d, matrix(d, h * CH))

    mine = pl.multiple_of(zero * rows, rows)
    sent = [0, 0]

    def drain(d, i):
        while sent[d] <= i:
            ring(d, sent[d]).wait_send()
            sent[d] += 1

    def receive(d, i):
        ring(d, i).wait_recv()
        pair(d, i).start()

    for i in range(own, pieces):
        if i == own:
            near_half(0)
        if i == own + CH:
            near_half(1)
        for d in range(2):
            drain(d, i - DEPTH)
            ring(d, i).start()
            if i < 2 * own:
                pair(d, i - own).start()
        if i == own + 1:
            for c in norm_z:
                c.start()
            for m in range(2):
                for t in range(columns // TILE):
                    at = slice(t * TILE, (t + 1) * TILE)
                    outs[m][pl.ds(mine, rows), at] = (whole[m, :, at] * inv[m, :, at]).astype(jnp.bfloat16)
        if i == own + 2:
            for m in range(2):
                block = outs[m].at[pl.ds(mine, rows)]
                remote(block, block, pair_send, pair_recv.at[m, 0], {"zero": peer}).start()
        if i == 2 * own:
            for c in norm_z:
                c.wait_recv()
            norm_pair.start()
        if i - LAG >= own:
            for d in range(2):
                receive(d, i - LAG)
    pl.when(z != nz - 1)(lambda: rest_ring(0).start())
    pl.when(z == 1)(lambda: rest_ring(1).start())
    norm_pair.wait_recv()
    for k in range(nz):
        for c in range(2):
            norm_out[2 * k + c : 2 * k + c + 1, :] = zbuf[c, k]
    for d in range(2):
        low(d).wait_send()
    for c in [first, *spread, back, *norm_z, norm_pair]:
        c.wait_send()
    for h in range(ny - 1):
        for e in range(2):

            @pl.when(gives(e, h))
            def _():
                norm_y(e, h).wait_send()

    def pair_got(m, slot):
        block = outs[m].at[pl.ds(0, rows)]
        remote(block, block, pair_send, pair_recv.at[m, slot], {"zero": peer}).wait_recv()

    early = [(m, slot) for m in range(2) for slot in range(nz) if slot not in (half - 1, half, half + 1)]
    for m, slot in early:
        pair_got(m, slot)
    for i in range(pieces - LAG, pieces):
        for d in range(2):
            receive(d, i)
    for d, here in ((0, z != 0), (1, z == 0)):

        @pl.when(here)
        def _():
            rest_ring(d).wait_recv()
            rest_pair(d).start()


    for slot in (half - 1, half, half + 1):
        for m in range(2):
            if (m, slot) not in early:
                pair_got(m, slot)
    for d in range(2):
        drain(d, pieces - 1)
    pl.when(z != nz - 1)(lambda: rest_ring(0).wait_send())
    pl.when(z == 1)(lambda: rest_ring(1).wait_send())
    remote(og, og, pair_send, pair_recv.at[0, 0], {"zero": peer}).wait_send()


def write_out(parts, *refs):
    ins, outs, (scratch, sem) = refs[:4], refs[4:9], refs[9:]
    size = ins[0].shape[0] // parts
    copies = [
        pltpu.make_async_copy(
            ins[m].at[pl.ds(i * size, size)], outs[m].at[pl.ds(i * size, size)], sem.at[m * parts + i]
        )
        for i in range(parts)
        for m in range(2)
    ]
    copies += [pltpu.make_async_copy(ins[2].at[m], outs[2 + m], sem.at[2 * parts + m]) for m in range(2)]
    for c in copies:
        c.start()
    scratch[...] = ins[3][...].astype(jnp.bfloat16)
    last = pltpu.make_async_copy(scratch, outs[4], sem.at[2 * parts + 2])
    last.start()
    for c in copies + [last]:
        c.wait()


def per_device(weight_gate, low_gate, high_gate, weight_up, low_up, high_up, norm_train, norm_step):
    devices, ny = lax.axis_size("zero"), lax.axis_size("cols")
    nz = devices // 2
    rows, columns = weight_gate.shape
    rank = low_gate.shape[1]
    share = norm_train.shape[0]
    tiles = columns // LANES
    f32, bf16 = jnp.float32, jnp.bfloat16
    hbm = pl.BlockSpec(memory_space=pltpu.HBM)
    vmem = pl.BlockSpec(memory_space=pltpu.VMEM)
    dma = pltpu.SemaphoreType.DMA
    serving_gate, serving_up, column, norm = pl.pallas_call(
        functools.partial(kernel, nz, ny),
        out_shape=(
            pltpu.VMEM((devices * rows, columns), bf16),
            pltpu.VMEM((devices * rows, columns), bf16),
            pltpu.VMEM((2, tiles, LANES), f32),
            pltpu.VMEM((devices, LANES), f32),
        ),
        in_specs=[hbm] * 8,
        out_specs=(vmem,) * 4,
        scratch_shapes=[
            pltpu.VMEM((2, rows, columns), bf16),
            pltpu.VMEM((2, rank, rows), bf16),
            pltpu.VMEM((2, rank, columns), bf16),
            pltpu.VMEM((2, 1, share), f32),
            pltpu.VMEM((2, 2, rows, columns), bf16),
            pltpu.VMEM((2, 2, rank, rows), bf16),
            pltpu.VMEM((2, rows, columns), f32),
            pltpu.VMEM((2, tiles, LANES), f32),
            pltpu.VMEM((tiles, LANES), f32),
            pltpu.VMEM((tiles, LANES), f32),
            pltpu.VMEM((nz, tiles, LANES), f32),
            pltpu.VMEM((2, 1, columns), f32),
            pltpu.VMEM((ny, 1, LANES), f32),
            pltpu.VMEM((2, nz, 1, LANES), f32),
            dma((8,)),
            dma((2, DEPTH)),
            dma((2, (nz - 1) * CH)),
            dma((2,)),
            dma((2,)),
            dma((2,)),
            dma((2,)),
            dma,
            dma((2, nz)),
            dma((nz + 1,)),
            dma((nz + 1,)),
            dma((2, ny - 1)),
            dma((2, ny - 1)),
            dma((nz,)),
            dma((nz,)),
            pltpu.SemaphoreType.REGULAR((3,)),
            pltpu.SemaphoreType.REGULAR((4,)),
        ],
        compiler_params=pltpu.CompilerParams(
            collective_id=0, has_side_effects=True, vmem_limit_bytes=47 << 20
        ),
    )(
        weight_gate, low_gate.T, high_gate, weight_up, low_up.T, high_up,
        norm_train.reshape(1, share), norm_step.reshape(1, share),
    )
    parts = 4
    serving_gate, serving_up, column_gate, column_up, norm = pl.pallas_call(
        functools.partial(write_out, parts),
        out_shape=(
            jax.ShapeDtypeStruct((devices * rows, columns), bf16),
            jax.ShapeDtypeStruct((devices * rows, columns), bf16),
            jax.ShapeDtypeStruct((tiles, LANES), f32),
            jax.ShapeDtypeStruct((tiles, LANES), f32),
            jax.ShapeDtypeStruct((devices, LANES), bf16),
        ),
        in_specs=[vmem] * 4,
        out_specs=(hbm,) * 5,
        scratch_shapes=[pltpu.VMEM((devices, LANES), bf16), dma((2 * parts + 3,))],
        compiler_params=pltpu.CompilerParams(vmem_limit_bytes=20 << 20),
    )(serving_gate, serving_up, column, norm)
    return (serving_gate, serving_up, column_gate.reshape(-1), column_up.reshape(-1), norm.reshape(-1))


def solution(mesh):
    in_specs = (
        P(("job", "zero"), "cols"),
        P(("job", "zero"), None),
        P("job", "cols"),
        P(("job", "zero"), "cols"),
        P(("job", "zero"), None),
        P("job", "cols"),
        P(("job", "zero", "cols")),
        P(("job", "zero", "cols")),
    )
    out_specs = (
        P("job", "cols"),
        P("job", "cols"),
        P(("job", "cols")),
        P(("job", "cols")),
        P("job"),
    )
    return jax.shard_map(
        per_device, mesh=mesh, in_specs=in_specs, out_specs=out_specs, check_vma=False
    )
```

```python
import functools

import jax
import jax.numpy as jnp
from jax import lax
from jax.experimental import pallas as pl
from jax.experimental.pallas import tpu as pltpu
from jax.sharding import PartitionSpec as P

mix_rate = 2.0
MESH = pl.DeviceIdType.MESH
CH = 4
TILE = 512
DEPTH = 8
LAG = 6
EARLY = (3, 2)
LANES = 128


def remote(src, dst, send_sem, recv_sem, device_id):
    return pltpu.make_async_remote_copy(
        src_ref=src, dst_ref=dst, send_sem=send_sem, recv_sem=recv_sem, device_id=device_id, device_id_type=MESH
    )


def kernel(
    nz, ny,
    wg_hbm, lg_hbm, hg_hbm, wu_hbm, lu_hbm, hu_hbm, nt_hbm, ns_hbm,
    og, ou, col_out, norm_out,
    w_in, l_in, h_in, n_in, raw, l_raw, whole, pmax, pget, cmax, cnear, allmax, inv, ybuf, zbuf,
    in_sem, ring_send, ring_recv, rest_send, rest_recv, low_send, low_recv, pair_send, pair_recv,
    max_send, max_recv, ny_send, ny_recv, nz_send, nz_recv, known, answer,
):
    zero, col = lax.axis_index("zero"), lax.axis_index("cols")
    z, core = zero // 2, zero % 2
    outs = (og, ou)
    rows, columns = w_in.shape[1:]
    step_rows = rows // CH
    half = nz // 2
    own = 2 * CH
    pieces = (2 * half - 1) * CH

    loads = [
        pltpu.make_async_copy(src, dst, in_sem.at[i])
        for i, (src, dst) in enumerate(
            (
                (wg_hbm, w_in.at[0]), (wu_hbm, w_in.at[1]), (lg_hbm, l_in.at[0]), (lu_hbm, l_in.at[1]),
                (hg_hbm, h_in.at[0]), (hu_hbm, h_in.at[1]), (nt_hbm, n_in.at[0]), (ns_hbm, n_in.at[1]),
            )
        )
    ]
    for c in loads:
        c.start()

    barrier = pltpu.get_barrier_semaphore()
    peer = zero + 1 - 2 * core
    to = ((z + 1) % nz * 2 + core, (z + nz - 1) % nz * 2 + core)
    others = [(z + d) % nz * 2 + core for d in range(1, nz)]
    sides = (col + 1 < ny, col > 0)
    beside = (lax.rem(col + 1, ny), lax.rem(col + ny - 1, ny))

    def signal(sem, axis, index):
        pl.semaphore_signal(sem, 1, device_id={axis: index}, device_id_type=MESH)

    low_end, high_end = z == 0, z == nz - 1
    pl.when(z < nz - 2)(lambda: signal(barrier, "zero", to[0]))
    pl.when(low_end | high_end)(lambda: signal(barrier, "zero", to[1]))
    pl.when(core == 1)(lambda: signal(barrier, "zero", peer))
    pl.when(sides[0])(lambda: signal(barrier, "cols", beside[0]))

    def greeted():
        count = sum(c.astype(jnp.int32) for c in (z > 0, z == nz - 2, core == 0, sides[1]))
        pl.when(count > 0)(lambda: pl.semaphore_wait(barrier, count))
        pl.when((z > 0) & (z < nz - 1))(lambda: signal(answer.at[0], "zero", to[1]))
        pl.when(z >= nz - 2)(lambda: signal(answer.at[1], "zero", to[0]))
        pl.when(core == 0)(lambda: signal(answer.at[2], "zero", peer))
        pl.when(sides[1])(lambda: signal(answer.at[3], "cols", beside[1]))

    def know(hops):
        pl.semaphore_wait(known.at[hops - 2], 2)

    def tell(hops):
        for t in to:
            pl.semaphore_signal(known.at[hops - 2], 1, device_id={"zero": t}, device_id_type=MESH)

    def merged(weights, low, m, at):
        return weights[:, at].astype(jnp.float32) + mix_rate * lax.dot_general(
            low[...], h_in[m, :, at], (((0,), (0,)), ((), ())), preferred_element_type=jnp.float32
        )

    def maxima(m):
        for t in range(columns // TILE):
            at = slice(t * TILE, (t + 1) * TILE)
            new = merged(w_in.at[m], l_in.at[m], m, at)
            whole[m, :, at] = new
            top = jnp.max(jnp.abs(new), axis=0, keepdims=True)
            for q in range(TILE // LANES):
                r = t * (TILE // LANES) + q
                pmax[m, r : r + 1, :] = top[:, q * LANES : (q + 1) * LANES]

    def block_rows(d, s):
        b = (z - s + nz) % nz if d == 0 else (z + s) % nz
        return (b * 2 + core) * rows

    def matrix(d, k):
        return k // CH if d == 0 else 1 - k // CH

    def chunk(k):
        return k * step_rows if k < CH else (own - 1 - k) * step_rows

    split = step_rows // 4 * 3

    def piece(d, i, hops):
        size = step_rows - split if i == pieces - 1 else step_rows
        at = pl.multiple_of(block_rows(d, i // own + hops) + chunk(i % own), step_rows // 4)
        return outs[matrix(d, i % own)].at[pl.ds(at, size)]

    def rest(via, m, hops):
        first_row = block_rows(via, half - 1 + hops) + chunk(CH - 1) + step_rows - split
        return outs[m].at[pl.ds(pl.multiple_of(first_row, step_rows // 4), split)]

    def rest_ring(via, m):
        ref = rest(via, m, 0)
        return remote(ref, ref, rest_send.at[via, m], rest_recv.at[via, m], {"zero": to[via]})

    def rest_pair(via, m):
        ref = rest(via, m, 1)
        return remote(ref, ref, pair_send, pair_recv.at[m, half], {"zero": peer})

    rest_out = ((0, 0, z != nz - 1), (1, 0, z == 1), (1, 1, z != half), (0, 1, z == half - 2))
    rest_in = ((0, 0, z != 0), (1, 0, z == 0), (1, 1, z != half - 1), (0, 1, z == half - 1))

    def ring(d, i):
        if i < own:
            m, at = matrix(d, i), pl.ds(chunk(i), step_rows)
            src = (wg_hbm, wu_hbm)[m].at[at] if i < EARLY[1] else w_in.at[m, at]
            dst = raw.at[d, m, at]
        else:
            src = dst = piece(d, i, 0)
        return remote(src, dst, ring_send.at[d, i % DEPTH], ring_recv.at[d, i], {"zero": to[d]})

    def pair(d, i):
        ref = piece(d, i, 1)
        s = i // own + 1
        slot = s if d == matrix(d, i % own) else (nz - s) % nz
        return remote(ref, ref, pair_send, pair_recv.at[matrix(d, i % own), slot], {"zero": peer})

    def low(d):
        return remote(l_in, l_raw.at[d], low_send.at[d], low_recv.at[d], {"zero": to[d]})

    def norm_y(e, h):
        row = ybuf.at[lax.rem(col + ny - h, ny) if e == 0 else lax.rem(col + h, ny)]
        return remote(row, row, ny_send.at[e, h], ny_recv.at[e, h], {"cols": beside[e]})

    def gives(e, h):
        return (sides[0] & (col >= h), sides[1] & (col + h < ny))[e]

    def gets(e, h):
        return (col >= h + 1, col + h + 1 < ny)[e]

    def norm_y_start(h):
        for e in range(2):

            @pl.when(gives(e, h))
            def _():
                norm_y(e, h).start()

    def norm_y_get(h):
        for e in range(2):

            @pl.when(gets(e, h))
            def _():
                norm_y(e, h).wait_recv()

    norm_z = [
        remote(zbuf.at[core, z], zbuf.at[core, z], nz_send.at[i], nz_recv.at[i], {"zero": t})
        for i, t in enumerate(others)
    ]
    norm_pair = remote(zbuf.at[core], zbuf.at[core], nz_send.at[nz - 1], nz_recv.at[nz - 1], {"zero": peer})

    greeted()

    def begin(d):
        for i in range(EARLY[1]):
            ring(d, i).start()

    def more(d, first, last):
        for i in range(first, last):
            ring(d, i).start()

    pl.when((z > 0) & (z < nz - 1))(lambda: begin(1))
    pl.when(z < nz - 2)(lambda: pl.semaphore_wait(answer.at[0], 1))
    begin(0)

    @pl.when(high_end)
    def _():
        pl.semaphore_wait(answer.at[1], 1)
        begin(1)

    pl.when(z > 0)(lambda: tell(2))
    for c in loads:
        c.wait()
    pl.when(z < half)(lambda: more(0, *EARLY[::-1]))
    pl.when((z > 0) & (z < half))(lambda: more(1, *EARLY[::-1]))
    gain = n_in[0] + n_in[1]
    ybuf[pl.ds(col, 1)] = jnp.concatenate([gain] * ny, axis=1)[None]
    maxima(0)

    @pl.when(low_end)
    def _():
        pl.semaphore_wait(answer.at[1], 1)
        tell(2)
        begin(1)

    for d in range(2):
        low(d).start()
    maxima(1)
    know(2)
    tell(3)
    pl.when(core == 1)(lambda: pl.semaphore_wait(answer.at[2], 1))
    pl.when(sides[0])(lambda: pl.semaphore_wait(answer.at[3], 1))

    first = remote(pmax.at[1 - core], pget, max_send.at[0], max_recv.at[0], {"zero": peer})
    first.start()
    norm_y_start(0)
    first.wait_recv()
    cmax[...] = jnp.maximum(pmax[core], pget[...])
    step_one = [remote(cmax, allmax.at[d], max_send.at[1 + d], max_recv.at[1 + d], {"zero": to[d]}) for d in range(2)]
    far = (others[2], others[nz - 4])
    step_two = [remote(cnear, allmax.at[2 + d], max_send.at[3 + d], max_recv.at[3 + d], {"zero": far[d]}) for d in range(2)]
    spread = step_one + step_two
    for c in step_one:
        c.start()

    def gap(d, early):
        more(d, early, early + 1)

    def fill(d, early):
        more(d, early + 1, own)

    def by_start(what):
        pl.when(z < half)(lambda: what(0, EARLY[0]))
        pl.when(z >= half)(lambda: what(0, EARLY[1]))
        pl.when((z > 0) & (z < half))(lambda: what(1, EARLY[0]))
        pl.when((z >= half) | low_end)(lambda: what(1, EARLY[1]))

    by_start(gap)
    know(3)
    for c in step_one:
        c.wait_recv()
    cnear[...] = jnp.maximum(jnp.maximum(cmax[...], allmax[0]), allmax[1])
    for c in step_two:
        c.start()
    by_start(fill)
    for h in range(1, ny - 1):
        norm_y_get(h - 1)
        norm_y_start(h)
    top = cnear[...]
    for d, c in enumerate(step_two):
        c.wait_recv()
        top = jnp.maximum(top, allmax[2 + d])
    col_out[pl.ds(core, 1)] = top[None]
    back = remote(col_out.at[core], col_out.at[core], max_send.at[nz], max_recv.at[nz], {"zero": peer})
    back.start()
    norm_y_get(ny - 2)
    lane = lax.broadcasted_iota(jnp.int32, (1, LANES), 1) // (LANES // ny)
    row = ybuf[0]
    for k in range(1, ny):
        row = jnp.where(lane == k, ybuf[k], row)
    zbuf[pl.ds(core, 1), pl.ds(z, 1)] = row[None, None]
    back.wait_recv()
    for m in range(2):
        for r in range(columns // LANES):
            inv[m, :, r * LANES : (r + 1) * LANES] = 1.0 / col_out[m, r : r + 1, :]

    def near(d, k):
        m, part = matrix(d, k), slice(chunk(k), chunk(k) + step_rows)
        first_row = pl.multiple_of(block_rows(d, 1) + chunk(k), step_rows)
        for t in range(columns // TILE):
            at = slice(t * TILE, (t + 1) * TILE)
            new = merged(raw.at[d, m, part], l_raw.at[d, m, :, part], m, at) * inv[m, :, at]
            outs[m][pl.ds(first_row, step_rows), at] = new.astype(jnp.bfloat16)

    mine = pl.multiple_of(zero * rows, rows)
    sent = [0, 0]

    def drain(d, i):
        while sent[d] <= i:
            ring(d, sent[d]).wait_send()
            sent[d] += 1

    def receive(d, i):
        ring(d, i).wait_recv()
        pair(d, i).start()

    for i in range(own, pieces):
        if i < 2 * own:
            for d in range(2):
                if i == own:
                    low(d).wait_recv()
                ring(d, i - own).wait_recv()
                near(d, i - own)
        for d in range(2):
            drain(d, i - DEPTH)
            ring(d, i).start()
            if i < 2 * own:
                pair(d, i - own).start()
        if i == own + 1:
            for c in norm_z:
                c.start()
            for m in range(2):
                for t in range(columns // TILE):
                    at = slice(t * TILE, (t + 1) * TILE)
                    outs[m][pl.ds(mine, rows), at] = (whole[m, :, at] * inv[m, :, at]).astype(jnp.bfloat16)
        if i == own + 2:
            for m in range(2):
                block = outs[m].at[pl.ds(mine, rows)]
                remote(block, block, pair_send, pair_recv.at[m, 0], {"zero": peer}).start()
        if i == 2 * own:
            for c in norm_z:
                c.wait_recv()
            norm_pair.start()
        if i - LAG >= own:
            for d in range(2):
                receive(d, i - LAG)
    for via, m, here in rest_out:
        pl.when(here)(lambda: rest_ring(via, m).start())
    norm_pair.wait_recv()
    for k in range(nz):
        for c in range(2):
            norm_out[2 * k + c : 2 * k + c + 1, :] = zbuf[c, k]
    for d in range(2):
        low(d).wait_send()
    for c in [first, *spread, back, *norm_z, norm_pair]:
        c.wait_send()
    for h in range(ny - 1):
        for e in range(2):

            @pl.when(gives(e, h))
            def _():
                norm_y(e, h).wait_send()

    def pair_got(m, slot):
        block = outs[m].at[pl.ds(0, rows)]
        remote(block, block, pair_send, pair_recv.at[m, slot], {"zero": peer}).wait_recv()

    early = [(m, slot) for m in range(2) for slot in range(nz) if slot not in (half - 1, half, half + 1)]
    for m, slot in early:
        pair_got(m, slot)
    for i in range(pieces - LAG, pieces):
        for d in range(2):
            receive(d, i)
    for via, m, here in rest_in:

        @pl.when(here)
        def _():
            rest_ring(via, m).wait_recv()
            rest_pair(via, m).start()


    for slot in (half - 1, half, half + 1):
        for m in range(2):
            if (m, slot) not in early:
                pair_got(m, slot)
    for d in range(2):
        drain(d, pieces - 1)
    for via, m, here in rest_out:
        pl.when(here)(lambda: rest_ring(via, m).wait_send())
    remote(og, og, pair_send, pair_recv.at[0, 0], {"zero": peer}).wait_send()


def write_out(parts, *refs):
    ins, outs, (scratch, sem) = refs[:4], refs[4:9], refs[9:]
    size = ins[0].shape[0] // parts
    copies = [
        pltpu.make_async_copy(
            ins[m].at[pl.ds(i * size, size)], outs[m].at[pl.ds(i * size, size)], sem.at[m * parts + i]
        )
        for i in range(parts)
        for m in range(2)
    ]
    copies += [pltpu.make_async_copy(ins[2].at[m], outs[2 + m], sem.at[2 * parts + m]) for m in range(2)]
    for c in copies:
        c.start()
    scratch[...] = ins[3][...].astype(jnp.bfloat16)
    last = pltpu.make_async_copy(scratch, outs[4], sem.at[2 * parts + 2])
    last.start()
    for c in copies + [last]:
        c.wait()


def per_device(weight_gate, low_gate, high_gate, weight_up, low_up, high_up, norm_train, norm_step):
    devices, ny = lax.axis_size("zero"), lax.axis_size("cols")
    nz = devices // 2
    rows, columns = weight_gate.shape
    rank = low_gate.shape[1]
    share = norm_train.shape[0]
    tiles = columns // LANES
    f32, bf16 = jnp.float32, jnp.bfloat16
    hbm = pl.BlockSpec(memory_space=pltpu.HBM)
    vmem = pl.BlockSpec(memory_space=pltpu.VMEM)
    dma = pltpu.SemaphoreType.DMA
    serving_gate, serving_up, column, norm = pl.pallas_call(
        functools.partial(kernel, nz, ny),
        out_shape=(
            pltpu.VMEM((devices * rows, columns), bf16),
            pltpu.VMEM((devices * rows, columns), bf16),
            pltpu.VMEM((2, tiles, LANES), f32),
            pltpu.VMEM((devices, LANES), f32),
        ),
        in_specs=[hbm] * 8,
        out_specs=(vmem,) * 4,
        scratch_shapes=[
            pltpu.VMEM((2, rows, columns), bf16),
            pltpu.VMEM((2, rank, rows), bf16),
            pltpu.VMEM((2, rank, columns), bf16),
            pltpu.VMEM((2, 1, share), f32),
            pltpu.VMEM((2, 2, rows, columns), bf16),
            pltpu.VMEM((2, 2, rank, rows), bf16),
            pltpu.VMEM((2, rows, columns), f32),
            pltpu.VMEM((2, tiles, LANES), f32),
            pltpu.VMEM((tiles, LANES), f32),
            pltpu.VMEM((tiles, LANES), f32),
            pltpu.VMEM((tiles, LANES), f32),
            pltpu.VMEM((4, tiles, LANES), f32),
            pltpu.VMEM((2, 1, columns), f32),
            pltpu.VMEM((ny, 1, LANES), f32),
            pltpu.VMEM((2, nz, 1, LANES), f32),
            dma((8,)),
            dma((2, DEPTH)),
            dma((2, (nz - 1) * CH)),
            dma((2, 2)),
            dma((2, 2)),
            dma((2,)),
            dma((2,)),
            dma,
            dma((2, nz)),
            dma((nz + 1,)),
            dma((nz + 1,)),
            dma((2, ny - 1)),
            dma((2, ny - 1)),
            dma((nz,)),
            dma((nz,)),
            pltpu.SemaphoreType.REGULAR((2,)),
            pltpu.SemaphoreType.REGULAR((4,)),
        ],
        compiler_params=pltpu.CompilerParams(
            collective_id=0, has_side_effects=True, vmem_limit_bytes=47 << 20
        ),
    )(
        weight_gate, low_gate.T, high_gate, weight_up, low_up.T, high_up,
        norm_train.reshape(1, share), norm_step.reshape(1, share),
    )
    parts = 4
    serving_gate, serving_up, column_gate, column_up, norm = pl.pallas_call(
        functools.partial(write_out, parts),
        out_shape=(
            jax.ShapeDtypeStruct((devices * rows, columns), bf16),
            jax.ShapeDtypeStruct((devices * rows, columns), bf16),
            jax.ShapeDtypeStruct((tiles, LANES), f32),
            jax.ShapeDtypeStruct((tiles, LANES), f32),
            jax.ShapeDtypeStruct((devices, LANES), bf16),
        ),
        in_specs=[vmem] * 4,
        out_specs=(hbm,) * 5,
        scratch_shapes=[pltpu.VMEM((devices, LANES), bf16), dma((2 * parts + 3,))],
        compiler_params=pltpu.CompilerParams(vmem_limit_bytes=20 << 20),
    )(serving_gate, serving_up, column, norm)
    return (serving_gate, serving_up, column_gate.reshape(-1), column_up.reshape(-1), norm.reshape(-1))


def solution(mesh):
    in_specs = (
        P(("job", "zero"), "cols"),
        P(("job", "zero"), None),
        P("job", "cols"),
        P(("job", "zero"), "cols"),
        P(("job", "zero"), None),
        P("job", "cols"),
        P(("job", "zero", "cols")),
        P(("job", "zero", "cols")),
    )
    out_specs = (
        P("job", "cols"),
        P("job", "cols"),
        P(("job", "cols")),
        P(("job", "cols")),
        P("job"),
    )
    return jax.shard_map(
        per_device, mesh=mesh, in_specs=in_specs, out_specs=out_specs, check_vma=False
    )
```

```python
import functools

import jax
import jax.numpy as jnp
from jax import lax
from jax.experimental import pallas as pl
from jax.experimental.pallas import tpu as pltpu
from jax.sharding import PartitionSpec as P

mix_rate = 2.0
MESH = pl.DeviceIdType.MESH
CH = 4
TILE = 512
DEPTH = 8
LAG = 6
EARLY = (3, 2)
LANES = 128


def remote(src, dst, send_sem, recv_sem, device_id):
    return pltpu.make_async_remote_copy(
        src_ref=src, dst_ref=dst, send_sem=send_sem, recv_sem=recv_sem, device_id=device_id, device_id_type=MESH
    )


def kernel(
    nz, ny,
    wg_hbm, lg_hbm, hg_hbm, wu_hbm, lu_hbm, hu_hbm, nt_hbm, ns_hbm,
    og, ou, col_out, norm_out,
    w_in, l_in, h_in, n_in, raw, l_raw, whole, pmax, pget, cmax, cnear, allmax, inv, ybuf, zbuf,
    in_sem, ring_send, ring_recv, rest_send, rest_recv, low_send, low_recv, pair_send, pair_recv,
    max_send, max_recv, ny_send, ny_recv, nz_send, nz_recv, known, answer,
):
    zero, col = lax.axis_index("zero"), lax.axis_index("cols")
    z, core = zero // 2, zero % 2
    outs = (og, ou)
    rows, columns = w_in.shape[1:]
    step_rows = rows // CH
    half = nz // 2
    own = 2 * CH
    pieces = (2 * half - 1) * CH

    loads = [
        pltpu.make_async_copy(src, dst, in_sem.at[i])
        for i, (src, dst) in enumerate(
            (
                (wg_hbm, w_in.at[0]), (wu_hbm, w_in.at[1]), (lg_hbm, l_in.at[0]), (lu_hbm, l_in.at[1]),
                (hg_hbm, h_in.at[0]), (hu_hbm, h_in.at[1]), (nt_hbm, n_in.at[0]), (ns_hbm, n_in.at[1]),
            )
        )
    ]
    for c in loads:
        c.start()

    barrier = pltpu.get_barrier_semaphore()
    peer = zero + 1 - 2 * core
    to = ((z + 1) % nz * 2 + core, (z + nz - 1) % nz * 2 + core)
    others = [(z + d) % nz * 2 + core for d in range(1, nz)]
    sides = (col + 1 < ny, col > 0)
    beside = (lax.rem(col + 1, ny), lax.rem(col + ny - 1, ny))

    def signal(sem, axis, index):
        pl.semaphore_signal(sem, 1, device_id={axis: index}, device_id_type=MESH)

    low_end, high_end = z == 0, z == nz - 1
    pl.when(z < nz - 2)(lambda: signal(barrier, "zero", to[0]))
    pl.when(low_end | high_end)(lambda: signal(barrier, "zero", to[1]))
    pl.when(core == 1)(lambda: signal(barrier, "zero", peer))
    pl.when(sides[0])(lambda: signal(barrier, "cols", beside[0]))

    def greeted():
        count = sum(c.astype(jnp.int32) for c in (z > 0, z == nz - 2, core == 0, sides[1]))
        pl.when(count > 0)(lambda: pl.semaphore_wait(barrier, count))
        pl.when((z > 0) & (z < nz - 1))(lambda: signal(answer.at[0], "zero", to[1]))
        pl.when(z >= nz - 2)(lambda: signal(answer.at[1], "zero", to[0]))
        pl.when(core == 0)(lambda: signal(answer.at[2], "zero", peer))
        pl.when(sides[1])(lambda: signal(answer.at[3], "cols", beside[1]))

    def know(hops):
        pl.semaphore_wait(known.at[hops - 2], 2)

    def tell(hops):
        for t in to:
            pl.semaphore_signal(known.at[hops - 2], 1, device_id={"zero": t}, device_id_type=MESH)

    def merged(weights, low, m, at):
        return weights[:, at].astype(jnp.float32) + mix_rate * lax.dot_general(
            low[...], h_in[m, :, at], (((0,), (0,)), ((), ())), preferred_element_type=jnp.float32
        )

    def maxima(m):
        for t in range(columns // TILE):
            at = slice(t * TILE, (t + 1) * TILE)
            new = merged(w_in.at[m], l_in.at[m], m, at)
            whole[m, :, at] = new
            top = jnp.max(jnp.abs(new), axis=0, keepdims=True)
            for q in range(TILE // LANES):
                r = t * (TILE // LANES) + q
                pmax[m, r : r + 1, :] = top[:, q * LANES : (q + 1) * LANES]

    def block_rows(d, s):
        b = (z - s + nz) % nz if d == 0 else (z + s) % nz
        return (b * 2 + core) * rows

    def matrix(d, k):
        return k // CH if d == 0 else 1 - k // CH

    def chunk(k):
        return k * step_rows if k < CH else (own - 1 - k) * step_rows

    split = step_rows // 4 * 3

    def piece(d, i, hops):
        size = step_rows - split if i == pieces - 1 else step_rows
        at = pl.multiple_of(block_rows(d, i // own + hops) + chunk(i % own), step_rows // 4)
        return outs[matrix(d, i % own)].at[pl.ds(at, size)]

    def rest(via, m, hops):
        first_row = block_rows(via, half - 1 + hops) + chunk(CH - 1) + step_rows - split
        return outs[m].at[pl.ds(pl.multiple_of(first_row, step_rows // 4), split)]

    def rest_ring(via, m):
        ref = rest(via, m, 0)
        return remote(ref, ref, rest_send.at[via, m], rest_recv.at[via, m], {"zero": to[via]})

    def rest_pair(via, m):
        ref = rest(via, m, 1)
        return remote(ref, ref, pair_send, pair_recv.at[m, half], {"zero": peer})

    rest_out = ((0, 0, z != nz - 1), (1, 0, z == 1), (1, 1, z != half), (0, 1, z == half - 2))
    rest_in = ((0, 0, z != 0), (1, 0, z == 0), (1, 1, z != half - 1), (0, 1, z == half - 1))

    def ring(d, i):
        if i < own:
            m, at = matrix(d, i), pl.ds(chunk(i), step_rows)
            src = (wg_hbm, wu_hbm)[m].at[at] if i < EARLY[1] else w_in.at[m, at]
            dst = raw.at[d, m, at]
        else:
            src = dst = piece(d, i, 0)
        return remote(src, dst, ring_send.at[d, i % DEPTH], ring_recv.at[d, i], {"zero": to[d]})

    def pair(d, i):
        ref = piece(d, i, 1)
        s = i // own + 1
        slot = s if d == matrix(d, i % own) else (nz - s) % nz
        return remote(ref, ref, pair_send, pair_recv.at[matrix(d, i % own), slot], {"zero": peer})

    def low(d):
        return remote(l_in, l_raw.at[d], low_send.at[d], low_recv.at[d], {"zero": to[d]})

    def norm_y(e, h):
        row = ybuf.at[lax.rem(col + ny - h, ny) if e == 0 else lax.rem(col + h, ny)]
        return remote(row, row, ny_send.at[e, h], ny_recv.at[e, h], {"cols": beside[e]})

    def gives(e, h):
        return (sides[0] & (col >= h), sides[1] & (col + h < ny))[e]

    def gets(e, h):
        return (col >= h + 1, col + h + 1 < ny)[e]

    def norm_y_start(h):
        for e in range(2):

            @pl.when(gives(e, h))
            def _():
                norm_y(e, h).start()

    def norm_y_get(h):
        for e in range(2):

            @pl.when(gets(e, h))
            def _():
                norm_y(e, h).wait_recv()

    norm_z = [
        remote(zbuf.at[core, z], zbuf.at[core, z], nz_send.at[i], nz_recv.at[i], {"zero": t})
        for i, t in enumerate(others)
    ]
    norm_pair = remote(zbuf.at[core], zbuf.at[core], nz_send.at[nz - 1], nz_recv.at[nz - 1], {"zero": peer})

    greeted()

    def begin(d):
        for i in range(EARLY[1]):
            ring(d, i).start()

    def more(d, first, last):
        for i in range(first, last):
            ring(d, i).start()

    pl.when((z > 0) & (z < nz - 1))(lambda: begin(1))
    pl.when(z < nz - 2)(lambda: pl.semaphore_wait(answer.at[0], 1))
    begin(0)

    @pl.when(high_end)
    def _():
        pl.semaphore_wait(answer.at[1], 1)
        begin(1)

    pl.when(z > 0)(lambda: tell(2))
    for c in loads:
        c.wait()
    pl.when(z < half - 1)(lambda: more(0, *EARLY[::-1]))
    pl.when((z > 0) & (z < half - 1))(lambda: more(1, *EARLY[::-1]))
    gain = n_in[0] + n_in[1]
    ybuf[pl.ds(col, 1)] = jnp.concatenate([gain] * ny, axis=1)[None]
    maxima(0)

    low(0).start()
    pl.when(z > 0)(lambda: low(1).start())
    maxima(1)

    @pl.when(low_end)
    def _():
        pl.semaphore_wait(answer.at[1], 1)
        tell(2)
        ring(1, 0).start()
        low(1).start()

    know(2)
    tell(3)
    pl.when(core == 1)(lambda: pl.semaphore_wait(answer.at[2], 1))
    pl.when(sides[0])(lambda: pl.semaphore_wait(answer.at[3], 1))

    first = remote(pmax.at[1 - core], pget, max_send.at[0], max_recv.at[0], {"zero": peer})
    first.start()
    norm_y_start(0)
    first.wait_recv()
    cmax[...] = jnp.maximum(pmax[core], pget[...])
    step_one = [remote(cmax, allmax.at[d], max_send.at[1 + d], max_recv.at[1 + d], {"zero": to[d]}) for d in range(2)]
    far = (others[2], others[nz - 4])
    step_two = [remote(cnear, allmax.at[2 + d], max_send.at[3 + d], max_recv.at[3 + d], {"zero": far[d]}) for d in range(2)]
    spread = step_one + step_two
    for c in step_one:
        c.start()

    def gap(d, early):
        more(d, early, early + 1)

    def fill(d, early):
        more(d, early + 1, own)

    def by_start(what):
        pl.when(z < half - 1)(lambda: what(0, EARLY[0]))
        pl.when(z >= half - 1)(lambda: what(0, EARLY[1]))
        pl.when((z > 0) & (z < half - 1))(lambda: what(1, EARLY[0]))
        pl.when(z >= half - 1)(lambda: what(1, EARLY[1]))
        pl.when(low_end)(lambda: what(1, 1))

    by_start(gap)
    know(3)
    for c in step_one:
        c.wait_recv()
    cnear[...] = jnp.maximum(jnp.maximum(cmax[...], allmax[0]), allmax[1])
    for c in step_two:
        c.start()
    by_start(fill)
    for h in range(1, ny - 1):
        norm_y_get(h - 1)
        norm_y_start(h)
    top = cnear[...]
    for d, c in enumerate(step_two):
        c.wait_recv()
        top = jnp.maximum(top, allmax[2 + d])
    col_out[pl.ds(core, 1)] = top[None]
    back = remote(col_out.at[core], col_out.at[core], max_send.at[nz], max_recv.at[nz], {"zero": peer})
    back.start()
    norm_y_get(ny - 2)
    lane = lax.broadcasted_iota(jnp.int32, (1, LANES), 1) // (LANES // ny)
    row = ybuf[0]
    for k in range(1, ny):
        row = jnp.where(lane == k, ybuf[k], row)
    zbuf[pl.ds(core, 1), pl.ds(z, 1)] = row[None, None]
    back.wait_recv()
    for m in range(2):
        for r in range(columns // LANES):
            inv[m, :, r * LANES : (r + 1) * LANES] = 1.0 / col_out[m, r : r + 1, :]

    def near(d, k):
        m, part = matrix(d, k), slice(chunk(k), chunk(k) + step_rows)
        first_row = pl.multiple_of(block_rows(d, 1) + chunk(k), step_rows)
        for t in range(columns // TILE):
            at = slice(t * TILE, (t + 1) * TILE)
            new = merged(raw.at[d, m, part], l_raw.at[d, m, :, part], m, at) * inv[m, :, at]
            outs[m][pl.ds(first_row, step_rows), at] = new.astype(jnp.bfloat16)

    mine = pl.multiple_of(zero * rows, rows)
    sent = [0, 0]

    def drain(d, i):
        while sent[d] <= i:
            ring(d, sent[d]).wait_send()
            sent[d] += 1

    def receive(d, i):
        ring(d, i).wait_recv()
        pair(d, i).start()

    for i in range(own, pieces):
        if i < 2 * own:
            for d in range(2):
                if i == own:
                    low(d).wait_recv()
                ring(d, i - own).wait_recv()
                near(d, i - own)
        if i == pieces - 1:
            for via, m, here in rest_out:
                pl.when(here)(lambda: rest_ring(via, m).start())
        for d in range(2):
            drain(d, i - DEPTH)
            ring(d, i).start()
            if i < 2 * own:
                pair(d, i - own).start()
        if i == own + 1:
            for c in norm_z:
                c.start()
            for m in range(2):
                for t in range(columns // TILE):
                    at = slice(t * TILE, (t + 1) * TILE)
                    outs[m][pl.ds(mine, rows), at] = (whole[m, :, at] * inv[m, :, at]).astype(jnp.bfloat16)
        if i == own + 2:
            for m in range(2):
                block = outs[m].at[pl.ds(mine, rows)]
                remote(block, block, pair_send, pair_recv.at[m, 0], {"zero": peer}).start()
        if i == 2 * own:
            for c in norm_z:
                c.wait_recv()
            norm_pair.start()
        if i - LAG >= own:
            for d in range(2):
                receive(d, i - LAG)
    norm_pair.wait_recv()
    for k in range(nz):
        for c in range(2):
            norm_out[2 * k + c : 2 * k + c + 1, :] = zbuf[c, k]
    for d in range(2):
        low(d).wait_send()
    for c in [first, *spread, back, *norm_z, norm_pair]:
        c.wait_send()
    for h in range(ny - 1):
        for e in range(2):

            @pl.when(gives(e, h))
            def _():
                norm_y(e, h).wait_send()

    def pair_got(m, slot):
        block = outs[m].at[pl.ds(0, rows)]
        remote(block, block, pair_send, pair_recv.at[m, slot], {"zero": peer}).wait_recv()

    early = [(m, slot) for m in range(2) for slot in range(nz) if slot not in (half - 1, half, half + 1)]
    for m, slot in early:
        pair_got(m, slot)
    for i in range(pieces - LAG, pieces - 1):
        for d in range(2):
            receive(d, i)
    for via, m, here in rest_in:

        @pl.when(here)
        def _():
            rest_ring(via, m).wait_recv()
            rest_pair(via, m).start()


    for d in range(2):
        receive(d, pieces - 1)
    for slot in (half - 1, half, half + 1):
        for m in range(2):
            if (m, slot) not in early:
                pair_got(m, slot)
    for d in range(2):
        drain(d, pieces - 1)
    for via, m, here in rest_out:
        pl.when(here)(lambda: rest_ring(via, m).wait_send())
    remote(og, og, pair_send, pair_recv.at[0, 0], {"zero": peer}).wait_send()


def write_out(parts, *refs):
    ins, outs, (scratch, sem) = refs[:4], refs[4:9], refs[9:]
    size = ins[0].shape[0] // parts
    copies = [
        pltpu.make_async_copy(
            ins[m].at[pl.ds(i * size, size)], outs[m].at[pl.ds(i * size, size)], sem.at[m * parts + i]
        )
        for i in range(parts)
        for m in range(2)
    ]
    copies += [pltpu.make_async_copy(ins[2].at[m], outs[2 + m], sem.at[2 * parts + m]) for m in range(2)]
    for c in copies:
        c.start()
    scratch[...] = ins[3][...].astype(jnp.bfloat16)
    last = pltpu.make_async_copy(scratch, outs[4], sem.at[2 * parts + 2])
    last.start()
    for c in copies + [last]:
        c.wait()


def per_device(weight_gate, low_gate, high_gate, weight_up, low_up, high_up, norm_train, norm_step):
    devices, ny = lax.axis_size("zero"), lax.axis_size("cols")
    nz = devices // 2
    rows, columns = weight_gate.shape
    rank = low_gate.shape[1]
    share = norm_train.shape[0]
    tiles = columns // LANES
    f32, bf16 = jnp.float32, jnp.bfloat16
    hbm = pl.BlockSpec(memory_space=pltpu.HBM)
    vmem = pl.BlockSpec(memory_space=pltpu.VMEM)
    dma = pltpu.SemaphoreType.DMA
    serving_gate, serving_up, column, norm = pl.pallas_call(
        functools.partial(kernel, nz, ny),
        out_shape=(
            pltpu.VMEM((devices * rows, columns), bf16),
            pltpu.VMEM((devices * rows, columns), bf16),
            pltpu.VMEM((2, tiles, LANES), f32),
            pltpu.VMEM((devices, LANES), f32),
        ),
        in_specs=[hbm] * 8,
        out_specs=(vmem,) * 4,
        scratch_shapes=[
            pltpu.VMEM((2, rows, columns), bf16),
            pltpu.VMEM((2, rank, rows), bf16),
            pltpu.VMEM((2, rank, columns), bf16),
            pltpu.VMEM((2, 1, share), f32),
            pltpu.VMEM((2, 2, rows, columns), bf16),
            pltpu.VMEM((2, 2, rank, rows), bf16),
            pltpu.VMEM((2, rows, columns), f32),
            pltpu.VMEM((2, tiles, LANES), f32),
            pltpu.VMEM((tiles, LANES), f32),
            pltpu.VMEM((tiles, LANES), f32),
            pltpu.VMEM((tiles, LANES), f32),
            pltpu.VMEM((4, tiles, LANES), f32),
            pltpu.VMEM((2, 1, columns), f32),
            pltpu.VMEM((ny, 1, LANES), f32),
            pltpu.VMEM((2, nz, 1, LANES), f32),
            dma((8,)),
            dma((2, DEPTH)),
            dma((2, (nz - 1) * CH)),
            dma((2, 2)),
            dma((2, 2)),
            dma((2,)),
            dma((2,)),
            dma,
            dma((2, nz)),
            dma((nz + 1,)),
            dma((nz + 1,)),
            dma((2, ny - 1)),
            dma((2, ny - 1)),
            dma((nz,)),
            dma((nz,)),
            pltpu.SemaphoreType.REGULAR((2,)),
            pltpu.SemaphoreType.REGULAR((4,)),
        ],
        compiler_params=pltpu.CompilerParams(
            collective_id=0, has_side_effects=True, vmem_limit_bytes=47 << 20
        ),
    )(
        weight_gate, low_gate.T, high_gate, weight_up, low_up.T, high_up,
        norm_train.reshape(1, share), norm_step.reshape(1, share),
    )
    parts = 4
    serving_gate, serving_up, column_gate, column_up, norm = pl.pallas_call(
        functools.partial(write_out, parts),
        out_shape=(
            jax.ShapeDtypeStruct((devices * rows, columns), bf16),
            jax.ShapeDtypeStruct((devices * rows, columns), bf16),
            jax.ShapeDtypeStruct((tiles, LANES), f32),
            jax.ShapeDtypeStruct((tiles, LANES), f32),
            jax.ShapeDtypeStruct((devices, LANES), bf16),
        ),
        in_specs=[vmem] * 4,
        out_specs=(hbm,) * 5,
        scratch_shapes=[pltpu.VMEM((devices, LANES), bf16), dma((2 * parts + 3,))],
        compiler_params=pltpu.CompilerParams(vmem_limit_bytes=20 << 20),
    )(serving_gate, serving_up, column, norm)
    return (serving_gate, serving_up, column_gate.reshape(-1), column_up.reshape(-1), norm.reshape(-1))


def solution(mesh):
    in_specs = (
        P(("job", "zero"), "cols"),
        P(("job", "zero"), None),
        P("job", "cols"),
        P(("job", "zero"), "cols"),
        P(("job", "zero"), None),
        P("job", "cols"),
        P(("job", "zero", "cols")),
        P(("job", "zero", "cols")),
    )
    out_specs = (
        P("job", "cols"),
        P("job", "cols"),
        P(("job", "cols")),
        P(("job", "cols")),
        P("job"),
    )
    return jax.shard_map(
        per_device, mesh=mesh, in_specs=in_specs, out_specs=out_specs, check_vma=False
    )
```

```python
import functools

import jax
import jax.numpy as jnp
from jax import lax
from jax.experimental import pallas as pl
from jax.experimental.pallas import tpu as pltpu
from jax.sharding import PartitionSpec as P

mix_rate = 2.0
MESH = pl.DeviceIdType.MESH
CH = 4
TILE = 512
DEPTH = 8
LAG = 6
EARLY = (3, 2)
LANES = 128


def remote(src, dst, send_sem, recv_sem, device_id):
    return pltpu.make_async_remote_copy(
        src_ref=src, dst_ref=dst, send_sem=send_sem, recv_sem=recv_sem, device_id=device_id, device_id_type=MESH
    )


def kernel(
    nz, ny,
    wg_hbm, lg_hbm, hg_hbm, wu_hbm, lu_hbm, hu_hbm, nt_hbm, ns_hbm,
    og, ou, col_out, norm_out,
    w_in, l_in, h_in, n_in, raw, l_raw, whole, pmax, pget, cmax, cnear, allmax, inv, ybuf, zbuf,
    in_sem, ring_send, ring_recv, rest_send, rest_recv, low_send, low_recv, pair_send, pair_recv,
    max_send, max_recv, ny_send, ny_recv, nz_send, nz_recv, known, answer,
):
    zero, col = lax.axis_index("zero"), lax.axis_index("cols")
    z, core = zero // 2, zero % 2
    outs = (og, ou)
    rows, columns = w_in.shape[1:]
    step_rows = rows // CH
    half = nz // 2
    own = 2 * CH
    pieces = (2 * half - 1) * CH

    loads = [
        pltpu.make_async_copy(src, dst, in_sem.at[i])
        for i, (src, dst) in enumerate(
            (
                (wg_hbm, w_in.at[0]), (wu_hbm, w_in.at[1]), (lg_hbm, l_in.at[0]), (lu_hbm, l_in.at[1]),
                (hg_hbm, h_in.at[0]), (hu_hbm, h_in.at[1]), (nt_hbm, n_in.at[0]), (ns_hbm, n_in.at[1]),
            )
        )
    ]
    def start_loads():
        for c in loads:
            c.start()

    barrier = pltpu.get_barrier_semaphore()
    peer = zero + 1 - 2 * core
    to = ((z + 1) % nz * 2 + core, (z + nz - 1) % nz * 2 + core)
    others = [(z + d) % nz * 2 + core for d in range(1, nz)]
    sides = (col + 1 < ny, col > 0)
    beside = (lax.rem(col + 1, ny), lax.rem(col + ny - 1, ny))

    def signal(sem, axis, index):
        pl.semaphore_signal(sem, 1, device_id={axis: index}, device_id_type=MESH)

    low_end, high_end = z == 0, z == nz - 1
    pl.when(z < nz - 2)(lambda: signal(barrier, "zero", to[0]))
    pl.when(low_end | high_end)(lambda: signal(barrier, "zero", to[1]))
    pl.when(core == 1)(lambda: signal(barrier, "zero", peer))
    pl.when(sides[0])(lambda: signal(barrier, "cols", beside[0]))

    feeds = (z == 1) | high_end
    pl.when(jnp.logical_not(feeds))(start_loads)

    def greeted():
        count = sum(c.astype(jnp.int32) for c in (z > 0, z == nz - 2, core == 0, sides[1]))
        pl.when(count > 0)(lambda: pl.semaphore_wait(barrier, count))
        pl.when((z > 0) & (z < nz - 1))(lambda: signal(answer.at[0], "zero", to[1]))
        pl.when(z >= nz - 2)(lambda: signal(answer.at[1], "zero", to[0]))
        pl.when(core == 0)(lambda: signal(answer.at[2], "zero", peer))
        pl.when(sides[1])(lambda: signal(answer.at[3], "cols", beside[1]))

    def know(hops):
        pl.semaphore_wait(known.at[hops - 2], 2)

    def tell(hops):
        for t in to:
            pl.semaphore_signal(known.at[hops - 2], 1, device_id={"zero": t}, device_id_type=MESH)

    def merged(weights, low, m, at):
        return weights[:, at].astype(jnp.float32) + mix_rate * lax.dot_general(
            low[...], h_in[m, :, at], (((0,), (0,)), ((), ())), preferred_element_type=jnp.float32
        )

    def maxima(m):
        for t in range(columns // TILE):
            at = slice(t * TILE, (t + 1) * TILE)
            new = merged(w_in.at[m], l_in.at[m], m, at)
            whole[m, :, at] = new
            top = jnp.max(jnp.abs(new), axis=0, keepdims=True)
            for q in range(TILE // LANES):
                r = t * (TILE // LANES) + q
                pmax[m, r : r + 1, :] = top[:, q * LANES : (q + 1) * LANES]

    def block_rows(d, s):
        b = (z - s + nz) % nz if d == 0 else (z + s) % nz
        return (b * 2 + core) * rows

    def matrix(d, k):
        return k // CH if d == 0 else 1 - k // CH

    def chunk(k):
        return k * step_rows if k < CH else (own - 1 - k) * step_rows

    split = step_rows // 4 * 3

    def piece(d, i, hops):
        size = step_rows - split if i == pieces - 1 else step_rows
        at = pl.multiple_of(block_rows(d, i // own + hops) + chunk(i % own), step_rows // 4)
        return outs[matrix(d, i % own)].at[pl.ds(at, size)]

    def rest(via, m, hops):
        first_row = block_rows(via, half - 1 + hops) + chunk(CH - 1) + step_rows - split
        return outs[m].at[pl.ds(pl.multiple_of(first_row, step_rows // 4), split)]

    def rest_ring(via, m):
        ref = rest(via, m, 0)
        return remote(ref, ref, rest_send.at[via, m], rest_recv.at[via, m], {"zero": to[via]})

    def rest_pair(via, m):
        ref = rest(via, m, 1)
        return remote(ref, ref, pair_send, pair_recv.at[m, half], {"zero": peer})

    rest_out = ((0, 0, z != nz - 1), (1, 0, z == 1), (1, 1, z != half), (0, 1, z == half - 2))
    rest_in = ((0, 0, z != 0), (1, 0, z == 0), (1, 1, z != half - 1), (0, 1, z == half - 1))

    def ring(d, i):
        if i < own:
            m, at = matrix(d, i), pl.ds(chunk(i), step_rows)
            src = (wg_hbm, wu_hbm)[m].at[at] if i < EARLY[1] else w_in.at[m, at]
            dst = raw.at[d, m, at]
        else:
            src = dst = piece(d, i, 0)
        return remote(src, dst, ring_send.at[d, i % DEPTH], ring_recv.at[d, i], {"zero": to[d]})

    def pair(d, i):
        ref = piece(d, i, 1)
        s = i // own + 1
        slot = s if d == matrix(d, i % own) else (nz - s) % nz
        return remote(ref, ref, pair_send, pair_recv.at[matrix(d, i % own), slot], {"zero": peer})

    def low(d):
        return remote(l_in, l_raw.at[d], low_send.at[d], low_recv.at[d], {"zero": to[d]})

    def norm_y(e, h):
        row = ybuf.at[lax.rem(col + ny - h, ny) if e == 0 else lax.rem(col + h, ny)]
        return remote(row, row, ny_send.at[e, h], ny_recv.at[e, h], {"cols": beside[e]})

    def gives(e, h):
        return (sides[0] & (col >= h), sides[1] & (col + h < ny))[e]

    def gets(e, h):
        return (col >= h + 1, col + h + 1 < ny)[e]

    def norm_y_start(h):
        for e in range(2):

            @pl.when(gives(e, h))
            def _():
                norm_y(e, h).start()

    def norm_y_get(h):
        for e in range(2):

            @pl.when(gets(e, h))
            def _():
                norm_y(e, h).wait_recv()

    norm_z = [
        remote(zbuf.at[core, z], zbuf.at[core, z], nz_send.at[i], nz_recv.at[i], {"zero": t})
        for i, t in enumerate(others)
    ]
    norm_pair = remote(zbuf.at[core], zbuf.at[core], nz_send.at[nz - 1], nz_recv.at[nz - 1], {"zero": peer})

    greeted()

    def begin(d):
        for i in range(EARLY[1]):
            ring(d, i).start()

    def more(d, first, last):
        for i in range(first, last):
            ring(d, i).start()

    pl.when((z > 0) & (z < nz - 1))(lambda: begin(1))
    pl.when(z == 1)(start_loads)
    pl.when(z < nz - 2)(lambda: pl.semaphore_wait(answer.at[0], 1))
    begin(0)
    pl.when(high_end)(start_loads)

    @pl.when(high_end)
    def _():
        pl.semaphore_wait(answer.at[1], 1)
        begin(1)

    pl.when(z > 0)(lambda: tell(2))
    for c in loads:
        c.wait()
    pl.when(z < half - 1)(lambda: more(0, *EARLY[::-1]))
    pl.when((z > 0) & (z < half - 1))(lambda: more(1, *EARLY[::-1]))
    gain = n_in[0] + n_in[1]
    ybuf[pl.ds(col, 1)] = jnp.concatenate([gain] * ny, axis=1)[None]
    maxima(0)

    low(0).start()
    pl.when(z > 0)(lambda: low(1).start())
    maxima(1)

    @pl.when(low_end)
    def _():
        pl.semaphore_wait(answer.at[1], 1)
        tell(2)
        ring(1, 0).start()
        low(1).start()

    know(2)
    tell(3)
    pl.when(core == 1)(lambda: pl.semaphore_wait(answer.at[2], 1))
    pl.when(sides[0])(lambda: pl.semaphore_wait(answer.at[3], 1))

    first = remote(pmax.at[1 - core], pget, max_send.at[0], max_recv.at[0], {"zero": peer})
    first.start()
    norm_y_start(0)
    first.wait_recv()
    cmax[...] = jnp.maximum(pmax[core], pget[...])
    step_one = [remote(cmax, allmax.at[d], max_send.at[1 + d], max_recv.at[1 + d], {"zero": to[d]}) for d in range(2)]
    far = (others[2], others[nz - 4])
    step_two = [remote(cnear, allmax.at[2 + d], max_send.at[3 + d], max_recv.at[3 + d], {"zero": far[d]}) for d in range(2)]
    spread = step_one + step_two
    for c in step_one:
        c.start()

    def gap(d, early):
        more(d, early, early + 1)

    def fill(d, early):
        more(d, early + 1, own)

    def by_start(what):
        pl.when(z < half - 1)(lambda: what(0, EARLY[0]))
        pl.when(z >= half - 1)(lambda: what(0, EARLY[1]))
        pl.when((z > 0) & (z < half - 1))(lambda: what(1, EARLY[0]))
        pl.when(z >= half - 1)(lambda: what(1, EARLY[1]))
        pl.when(low_end)(lambda: what(1, 1))

    by_start(gap)
    know(3)
    for c in step_one:
        c.wait_recv()
    cnear[...] = jnp.maximum(jnp.maximum(cmax[...], allmax[0]), allmax[1])
    for c in step_two:
        c.start()
    by_start(fill)
    for h in range(1, ny - 1):
        norm_y_get(h - 1)
        norm_y_start(h)
    top = cnear[...]
    for d, c in enumerate(step_two):
        c.wait_recv()
        top = jnp.maximum(top, allmax[2 + d])
    col_out[pl.ds(core, 1)] = top[None]
    back = remote(col_out.at[core], col_out.at[core], max_send.at[nz], max_recv.at[nz], {"zero": peer})
    back.start()
    norm_y_get(ny - 2)
    lane = lax.broadcasted_iota(jnp.int32, (1, LANES), 1) // (LANES // ny)
    row = ybuf[0]
    for k in range(1, ny):
        row = jnp.where(lane == k, ybuf[k], row)
    zbuf[pl.ds(core, 1), pl.ds(z, 1)] = row[None, None]
    back.wait_recv()
    for m in range(2):
        for r in range(columns // LANES):
            inv[m, :, r * LANES : (r + 1) * LANES] = 1.0 / col_out[m, r : r + 1, :]

    def near(d, k):
        m, part = matrix(d, k), slice(chunk(k), chunk(k) + step_rows)
        first_row = pl.multiple_of(block_rows(d, 1) + chunk(k), step_rows)
        for t in range(columns // TILE):
            at = slice(t * TILE, (t + 1) * TILE)
            new = merged(raw.at[d, m, part], l_raw.at[d, m, :, part], m, at) * inv[m, :, at]
            outs[m][pl.ds(first_row, step_rows), at] = new.astype(jnp.bfloat16)

    mine = pl.multiple_of(zero * rows, rows)
    sent = [0, 0]

    def drain(d, i):
        while sent[d] <= i:
            ring(d, sent[d]).wait_send()
            sent[d] += 1

    def receive(d, i):
        ring(d, i).wait_recv()
        pair(d, i).start()

    for i in range(own, pieces):
        if i < 2 * own:
            for d in range(2):
                if i == own:
                    low(d).wait_recv()
                ring(d, i - own).wait_recv()
                near(d, i - own)
        if i == pieces - 1:
            for via, m, here in rest_out:
                pl.when(here)(lambda: rest_ring(via, m).start())
        for d in range(2):
            drain(d, i - DEPTH)
            ring(d, i).start()
            if i < 2 * own:
                pair(d, i - own).start()
        if i == own + 1:
            for c in norm_z:
                c.start()
            for m in range(2):
                for t in range(columns // TILE):
                    at = slice(t * TILE, (t + 1) * TILE)
                    outs[m][pl.ds(mine, rows), at] = (whole[m, :, at] * inv[m, :, at]).astype(jnp.bfloat16)
        if i == own + 2:
            for m in range(2):
                block = outs[m].at[pl.ds(mine, rows)]
                remote(block, block, pair_send, pair_recv.at[m, 0], {"zero": peer}).start()
        if i == 2 * own:
            for c in norm_z:
                c.wait_recv()
            norm_pair.start()
        if i - LAG >= own:
            for d in range(2):
                receive(d, i - LAG)
    norm_pair.wait_recv()
    for k in range(nz):
        for c in range(2):
            norm_out[2 * k + c : 2 * k + c + 1, :] = zbuf[c, k]
    for d in range(2):
        low(d).wait_send()
    for c in [first, *spread, back, *norm_z, norm_pair]:
        c.wait_send()
    for h in range(ny - 1):
        for e in range(2):

            @pl.when(gives(e, h))
            def _():
                norm_y(e, h).wait_send()

    def pair_got(m, slot):
        block = outs[m].at[pl.ds(0, rows)]
        remote(block, block, pair_send, pair_recv.at[m, slot], {"zero": peer}).wait_recv()

    early = [(m, slot) for m in range(2) for slot in range(nz) if slot not in (half - 1, half, half + 1)]
    for m, slot in early:
        pair_got(m, slot)
    for i in range(pieces - LAG, pieces - 1):
        for d in range(2):
            receive(d, i)
    for via, m, here in rest_in:

        @pl.when(here)
        def _():
            rest_ring(via, m).wait_recv()
            rest_pair(via, m).start()


    for d in range(2):
        receive(d, pieces - 1)
    for slot in (half - 1, half, half + 1):
        for m in range(2):
            if (m, slot) not in early:
                pair_got(m, slot)
    for d in range(2):
        drain(d, pieces - 1)
    for via, m, here in rest_out:
        pl.when(here)(lambda: rest_ring(via, m).wait_send())
    remote(og, og, pair_send, pair_recv.at[0, 0], {"zero": peer}).wait_send()


def write_out(parts, *refs):
    ins, outs, (scratch, sem) = refs[:4], refs[4:9], refs[9:]
    size = ins[0].shape[0] // parts
    copies = [
        pltpu.make_async_copy(
            ins[m].at[pl.ds(i * size, size)], outs[m].at[pl.ds(i * size, size)], sem.at[m * parts + i]
        )
        for i in range(parts)
        for m in range(2)
    ]
    copies += [pltpu.make_async_copy(ins[2].at[m], outs[2 + m], sem.at[2 * parts + m]) for m in range(2)]
    for c in copies:
        c.start()
    scratch[...] = ins[3][...].astype(jnp.bfloat16)
    last = pltpu.make_async_copy(scratch, outs[4], sem.at[2 * parts + 2])
    last.start()
    for c in copies + [last]:
        c.wait()


def per_device(weight_gate, low_gate, high_gate, weight_up, low_up, high_up, norm_train, norm_step):
    devices, ny = lax.axis_size("zero"), lax.axis_size("cols")
    nz = devices // 2
    rows, columns = weight_gate.shape
    rank = low_gate.shape[1]
    share = norm_train.shape[0]
    tiles = columns // LANES
    f32, bf16 = jnp.float32, jnp.bfloat16
    hbm = pl.BlockSpec(memory_space=pltpu.HBM)
    vmem = pl.BlockSpec(memory_space=pltpu.VMEM)
    dma = pltpu.SemaphoreType.DMA
    serving_gate, serving_up, column, norm = pl.pallas_call(
        functools.partial(kernel, nz, ny),
        out_shape=(
            pltpu.VMEM((devices * rows, columns), bf16),
            pltpu.VMEM((devices * rows, columns), bf16),
            pltpu.VMEM((2, tiles, LANES), f32),
            pltpu.VMEM((devices, LANES), f32),
        ),
        in_specs=[hbm] * 8,
        out_specs=(vmem,) * 4,
        scratch_shapes=[
            pltpu.VMEM((2, rows, columns), bf16),
            pltpu.VMEM((2, rank, rows), bf16),
            pltpu.VMEM((2, rank, columns), bf16),
            pltpu.VMEM((2, 1, share), f32),
            pltpu.VMEM((2, 2, rows, columns), bf16),
            pltpu.VMEM((2, 2, rank, rows), bf16),
            pltpu.VMEM((2, rows, columns), f32),
            pltpu.VMEM((2, tiles, LANES), f32),
            pltpu.VMEM((tiles, LANES), f32),
            pltpu.VMEM((tiles, LANES), f32),
            pltpu.VMEM((tiles, LANES), f32),
            pltpu.VMEM((4, tiles, LANES), f32),
            pltpu.VMEM((2, 1, columns), f32),
            pltpu.VMEM((ny, 1, LANES), f32),
            pltpu.VMEM((2, nz, 1, LANES), f32),
            dma((8,)),
            dma((2, DEPTH)),
            dma((2, (nz - 1) * CH)),
            dma((2, 2)),
            dma((2, 2)),
            dma((2,)),
            dma((2,)),
            dma,
            dma((2, nz)),
            dma((nz + 1,)),
            dma((nz + 1,)),
            dma((2, ny - 1)),
            dma((2, ny - 1)),
            dma((nz,)),
            dma((nz,)),
            pltpu.SemaphoreType.REGULAR((2,)),
            pltpu.SemaphoreType.REGULAR((4,)),
        ],
        compiler_params=pltpu.CompilerParams(
            collective_id=0, has_side_effects=True, vmem_limit_bytes=47 << 20
        ),
    )(
        weight_gate, low_gate.T, high_gate, weight_up, low_up.T, high_up,
        norm_train.reshape(1, share), norm_step.reshape(1, share),
    )
    parts = 4
    serving_gate, serving_up, column_gate, column_up, norm = pl.pallas_call(
        functools.partial(write_out, parts),
        out_shape=(
            jax.ShapeDtypeStruct((devices * rows, columns), bf16),
            jax.ShapeDtypeStruct((devices * rows, columns), bf16),
            jax.ShapeDtypeStruct((tiles, LANES), f32),
            jax.ShapeDtypeStruct((tiles, LANES), f32),
            jax.ShapeDtypeStruct((devices, LANES), bf16),
        ),
        in_specs=[vmem] * 4,
        out_specs=(hbm,) * 5,
        scratch_shapes=[pltpu.VMEM((devices, LANES), bf16), dma((2 * parts + 3,))],
        compiler_params=pltpu.CompilerParams(vmem_limit_bytes=20 << 20),
    )(serving_gate, serving_up, column, norm)
    return (serving_gate, serving_up, column_gate.reshape(-1), column_up.reshape(-1), norm.reshape(-1))


def solution(mesh):
    in_specs = (
        P(("job", "zero"), "cols"),
        P(("job", "zero"), None),
        P("job", "cols"),
        P(("job", "zero"), "cols"),
        P(("job", "zero"), None),
        P("job", "cols"),
        P(("job", "zero", "cols")),
        P(("job", "zero", "cols")),
    )
    out_specs = (
        P("job", "cols"),
        P("job", "cols"),
        P(("job", "cols")),
        P(("job", "cols")),
        P("job"),
    )
    return jax.shard_map(
        per_device, mesh=mesh, in_specs=in_specs, out_specs=out_specs, check_vma=False
    )
```

```python
import functools

import jax
import jax.numpy as jnp
from jax import lax
from jax.experimental import pallas as pl
from jax.experimental.pallas import tpu as pltpu
from jax.sharding import PartitionSpec as P

mix_rate = 2.0
MESH = pl.DeviceIdType.MESH
CH = 4
TILE = 512
DEPTH = 8
LAG = 6
EARLY = (3, 2)
LANES = 128


def remote(src, dst, send_sem, recv_sem, device_id):
    return pltpu.make_async_remote_copy(
        src_ref=src, dst_ref=dst, send_sem=send_sem, recv_sem=recv_sem, device_id=device_id, device_id_type=MESH
    )


def kernel(
    nz, ny,
    wg_hbm, lg_hbm, hg_hbm, wu_hbm, lu_hbm, hu_hbm, nt_hbm, ns_hbm,
    og, ou, col_out, norm_out,
    w_in, l_in, h_in, n_in, raw, l_raw, whole, pmax, pget, cmax, cnear, allmax, inv, ybuf, zbuf,
    in_sem, ring_send, ring_recv, rest_send, rest_recv, low_send, low_recv, pair_send, pair_recv,
    max_send, max_recv, ny_send, ny_recv, nz_send, nz_recv, known, answer,
):
    zero, col = lax.axis_index("zero"), lax.axis_index("cols")
    z, core = zero // 2, zero % 2
    outs = (og, ou)
    rows, columns = w_in.shape[1:]
    step_rows = rows // CH
    half = nz // 2
    own = 2 * CH
    pieces = (2 * half - 1) * CH

    loads = [
        pltpu.make_async_copy(src, dst, in_sem.at[i])
        for i, (src, dst) in enumerate(
            (
                (wg_hbm, w_in.at[0]), (wu_hbm, w_in.at[1]), (lg_hbm, l_in.at[0]), (lu_hbm, l_in.at[1]),
                (hg_hbm, h_in.at[0]), (hu_hbm, h_in.at[1]), (nt_hbm, n_in.at[0]), (ns_hbm, n_in.at[1]),
            )
        )
    ]
    barrier = pltpu.get_barrier_semaphore()
    peer = zero + 1 - 2 * core
    to = ((z + 1) % nz * 2 + core, (z + nz - 1) % nz * 2 + core)
    others = [(z + d) % nz * 2 + core for d in range(1, nz)]
    sides = (col + 1 < ny, col > 0)
    beside = (lax.rem(col + 1, ny), lax.rem(col + ny - 1, ny))

    def signal(sem, axis, index):
        pl.semaphore_signal(sem, 1, device_id={axis: index}, device_id_type=MESH)

    low_end, high_end = z == 0, z == nz - 1
    pl.when(z < nz - 2)(lambda: signal(barrier, "zero", to[0]))
    pl.when(low_end | high_end)(lambda: signal(barrier, "zero", to[1]))
    pl.when(core == 1)(lambda: signal(barrier, "zero", peer))
    pl.when(sides[0])(lambda: signal(barrier, "cols", beside[0]))

    for c in loads:
        c.start()

    def greeted():
        count = sum(c.astype(jnp.int32) for c in (z > 0, z == nz - 2, core == 0, sides[1]))
        pl.when(count > 0)(lambda: pl.semaphore_wait(barrier, count))
        pl.when((z > 0) & (z < nz - 1))(lambda: signal(answer.at[0], "zero", to[1]))
        pl.when(z >= nz - 2)(lambda: signal(answer.at[1], "zero", to[0]))
        pl.when(core == 0)(lambda: signal(answer.at[2], "zero", peer))
        pl.when(sides[1])(lambda: signal(answer.at[3], "cols", beside[1]))

    def know(hops):
        pl.semaphore_wait(known.at[hops - 2], 2)

    def tell(hops):
        for t in to:
            pl.semaphore_signal(known.at[hops - 2], 1, device_id={"zero": t}, device_id_type=MESH)

    def merged(weights, low, m, at):
        return weights[:, at].astype(jnp.float32) + mix_rate * lax.dot_general(
            low[...], h_in[m, :, at], (((0,), (0,)), ((), ())), preferred_element_type=jnp.float32
        )

    def maxima(m):
        for t in range(columns // TILE):
            at = slice(t * TILE, (t + 1) * TILE)
            new = merged(w_in.at[m], l_in.at[m], m, at)
            whole[m, :, at] = new
            top = jnp.max(jnp.abs(new), axis=0, keepdims=True)
            for q in range(TILE // LANES):
                r = t * (TILE // LANES) + q
                pmax[m, r : r + 1, :] = top[:, q * LANES : (q + 1) * LANES]

    def block_rows(d, s):
        b = (z - s + nz) % nz if d == 0 else (z + s) % nz
        return (b * 2 + core) * rows

    def matrix(d, k):
        return k // CH if d == 0 else 1 - k // CH

    def chunk(k):
        return k * step_rows if k < CH else (own - 1 - k) * step_rows

    split = step_rows // 4 * 3

    def piece(d, i, hops):
        size = step_rows - split if i == pieces - 1 else step_rows
        at = pl.multiple_of(block_rows(d, i // own + hops) + chunk(i % own), step_rows // 4)
        return outs[matrix(d, i % own)].at[pl.ds(at, size)]

    def rest(via, m, hops):
        first_row = block_rows(via, half - 1 + hops) + chunk(CH - 1) + step_rows - split
        return outs[m].at[pl.ds(pl.multiple_of(first_row, step_rows // 4), split)]

    def rest_ring(via, m):
        ref = rest(via, m, 0)
        return remote(ref, ref, rest_send.at[via, m], rest_recv.at[via, m], {"zero": to[via]})

    def rest_pair(via, m):
        ref = rest(via, m, 1)
        return remote(ref, ref, pair_send, pair_recv.at[m, half], {"zero": peer})

    rest_out = ((0, 0, z != nz - 1), (1, 0, z == 1), (1, 1, z != half), (0, 1, z == half - 2))
    rest_in = ((0, 0, z != 0), (1, 0, z == 0), (1, 1, z != half - 1), (0, 1, z == half - 1))

    def ring(d, i):
        if i < own:
            m, at = matrix(d, i), pl.ds(chunk(i), step_rows)
            src = (wg_hbm, wu_hbm)[m].at[at] if i < EARLY[1] else w_in.at[m, at]
            dst = raw.at[d, m, at]
        else:
            src = dst = piece(d, i, 0)
        return remote(src, dst, ring_send.at[d, i % DEPTH], ring_recv.at[d, i], {"zero": to[d]})

    def pair(d, i):
        ref = piece(d, i, 1)
        s = i // own + 1
        slot = s if d == matrix(d, i % own) else (nz - s) % nz
        return remote(ref, ref, pair_send, pair_recv.at[matrix(d, i % own), slot], {"zero": peer})

    def low(d):
        return remote(l_in, l_raw.at[d], low_send.at[d], low_recv.at[d], {"zero": to[d]})

    def norm_y(e, h):
        row = ybuf.at[lax.rem(col + ny - h, ny) if e == 0 else lax.rem(col + h, ny)]
        return remote(row, row, ny_send.at[e, h], ny_recv.at[e, h], {"cols": beside[e]})

    def gives(e, h):
        return (sides[0] & (col >= h), sides[1] & (col + h < ny))[e]

    def gets(e, h):
        return (col >= h + 1, col + h + 1 < ny)[e]

    def norm_y_start(h):
        for e in range(2):

            @pl.when(gives(e, h))
            def _():
                norm_y(e, h).start()

    def norm_y_get(h):
        for e in range(2):

            @pl.when(gets(e, h))
            def _():
                norm_y(e, h).wait_recv()

    norm_z = [
        remote(zbuf.at[core, z], zbuf.at[core, z], nz_send.at[i], nz_recv.at[i], {"zero": t})
        for i, t in enumerate(others)
    ]
    norm_pair = remote(zbuf.at[core], zbuf.at[core], nz_send.at[nz - 1], nz_recv.at[nz - 1], {"zero": peer})

    greeted()

    def begin(d):
        for i in range(EARLY[1]):
            ring(d, i).start()

    def more(d, first, last):
        for i in range(first, last):
            ring(d, i).start()

    pl.when((z > 0) & (z < nz - 1))(lambda: begin(1))
    pl.when(z < nz - 2)(lambda: pl.semaphore_wait(answer.at[0], 1))
    begin(0)

    @pl.when(high_end)
    def _():
        pl.semaphore_wait(answer.at[1], 1)
        begin(1)

    pl.when(z > 0)(lambda: tell(2))
    for c in loads:
        c.wait()
    pl.when(z < half - 1)(lambda: more(0, *EARLY[::-1]))
    pl.when((z > 0) & (z < half - 1))(lambda: more(1, *EARLY[::-1]))
    gain = n_in[0] + n_in[1]
    ybuf[pl.ds(col, 1)] = jnp.concatenate([gain] * ny, axis=1)[None]
    maxima(0)

    low(0).start()
    pl.when(z > 0)(lambda: low(1).start())
    maxima(1)

    @pl.when(low_end)
    def _():
        pl.semaphore_wait(answer.at[1], 1)
        tell(2)
        ring(1, 0).start()
        low(1).start()

    know(2)
    tell(3)
    pl.when(core == 1)(lambda: pl.semaphore_wait(answer.at[2], 1))
    pl.when(sides[0])(lambda: pl.semaphore_wait(answer.at[3], 1))

    first = remote(pmax.at[1 - core], pget, max_send.at[0], max_recv.at[0], {"zero": peer})
    first.start()
    norm_y_start(0)
    first.wait_recv()
    cmax[...] = jnp.maximum(pmax[core], pget[...])
    step_one = [remote(cmax, allmax.at[d], max_send.at[1 + d], max_recv.at[1 + d], {"zero": to[d]}) for d in range(2)]
    far = (others[2], others[nz - 4])
    step_two = [remote(cnear, allmax.at[2 + d], max_send.at[3 + d], max_recv.at[3 + d], {"zero": far[d]}) for d in range(2)]
    spread = step_one + step_two
    for c in step_one:
        c.start()

    def gap(d, early):
        more(d, early, early + 1)

    def fill(d, early):
        more(d, early + 1, own)

    def by_start(what):
        pl.when(z < half - 1)(lambda: what(0, EARLY[0]))
        pl.when(z >= half - 1)(lambda: what(0, EARLY[1]))
        pl.when((z > 0) & (z < half - 1))(lambda: what(1, EARLY[0]))
        pl.when(z >= half - 1)(lambda: what(1, EARLY[1]))
        pl.when(low_end)(lambda: what(1, 1))

    by_start(gap)
    know(3)
    for c in step_one:
        c.wait_recv()
    cnear[...] = jnp.maximum(jnp.maximum(cmax[...], allmax[0]), allmax[1])
    for c in step_two:
        c.start()
    by_start(fill)
    for h in range(1, ny - 1):
        norm_y_get(h - 1)
        norm_y_start(h)
    top = cnear[...]
    for d, c in enumerate(step_two):
        c.wait_recv()
        top = jnp.maximum(top, allmax[2 + d])
    col_out[pl.ds(core, 1)] = top[None]
    back = remote(col_out.at[core], col_out.at[core], max_send.at[nz], max_recv.at[nz], {"zero": peer})
    back.start()
    norm_y_get(ny - 2)
    lane = lax.broadcasted_iota(jnp.int32, (1, LANES), 1) // (LANES // ny)
    row = ybuf[0]
    for k in range(1, ny):
        row = jnp.where(lane == k, ybuf[k], row)
    zbuf[pl.ds(core, 1), pl.ds(z, 1)] = row[None, None]
    back.wait_recv()
    for m in range(2):
        for r in range(columns // LANES):
            inv[m, :, r * LANES : (r + 1) * LANES] = 1.0 / col_out[m, r : r + 1, :]

    def near(d, k):
        m, part = matrix(d, k), slice(chunk(k), chunk(k) + step_rows)
        first_row = pl.multiple_of(block_rows(d, 1) + chunk(k), step_rows)
        for t in range(columns // TILE):
            at = slice(t * TILE, (t + 1) * TILE)
            new = merged(raw.at[d, m, part], l_raw.at[d, m, :, part], m, at) * inv[m, :, at]
            outs[m][pl.ds(first_row, step_rows), at] = new.astype(jnp.bfloat16)

    mine = pl.multiple_of(zero * rows, rows)
    sent = [0, 0]

    def drain(d, i):
        while sent[d] <= i:
            ring(d, sent[d]).wait_send()
            sent[d] += 1

    def receive(d, i):
        ring(d, i).wait_recv()
        pair(d, i).start()

    for i in range(own, pieces):
        if i < 2 * own:
            for d in range(2):
                if i == own:
                    low(d).wait_recv()
                ring(d, i - own).wait_recv()
                near(d, i - own)
        if i == pieces - 1:
            for via, m, here in rest_out:
                pl.when(here)(lambda: rest_ring(via, m).start())
        for d in range(2):
            drain(d, i - DEPTH)
            ring(d, i).start()
            if i < 2 * own:
                pair(d, i - own).start()
        if i == own + 1:
            for c in norm_z:
                c.start()
            for m in range(2):
                for t in range(columns // TILE):
                    at = slice(t * TILE, (t + 1) * TILE)
                    outs[m][pl.ds(mine, rows), at] = (whole[m, :, at] * inv[m, :, at]).astype(jnp.bfloat16)
        if i == own + 2:
            for m in range(2):
                block = outs[m].at[pl.ds(mine, rows)]
                remote(block, block, pair_send, pair_recv.at[m, 0], {"zero": peer}).start()
        if i == 2 * own:
            for c in norm_z:
                c.wait_recv()
            norm_pair.start()
        if i - LAG >= own:
            for d in range(2):
                receive(d, i - LAG)
    norm_pair.wait_recv()
    for k in range(nz):
        for c in range(2):
            norm_out[2 * k + c : 2 * k + c + 1, :] = zbuf[c, k]
    for d in range(2):
        low(d).wait_send()
    for c in [first, *spread, back, *norm_z, norm_pair]:
        c.wait_send()
    for h in range(ny - 1):
        for e in range(2):

            @pl.when(gives(e, h))
            def _():
                norm_y(e, h).wait_send()

    def pair_got(m, slot):
        block = outs[m].at[pl.ds(0, rows)]
        remote(block, block, pair_send, pair_recv.at[m, slot], {"zero": peer}).wait_recv()

    early = [(m, slot) for m in range(2) for slot in range(nz) if slot not in (half - 1, half, half + 1)]
    for m, slot in early:
        pair_got(m, slot)
    for i in range(pieces - LAG, pieces - 1):
        for d in range(2):
            receive(d, i)
    for via, m, here in rest_in:

        @pl.when(here)
        def _():
            rest_ring(via, m).wait_recv()
            rest_pair(via, m).start()


    for d in range(2):
        receive(d, pieces - 1)
    for slot in (half - 1, half, half + 1):
        for m in range(2):
            if (m, slot) not in early:
                pair_got(m, slot)
    for d in range(2):
        drain(d, pieces - 1)
    for via, m, here in rest_out:
        pl.when(here)(lambda: rest_ring(via, m).wait_send())
    remote(og, og, pair_send, pair_recv.at[0, 0], {"zero": peer}).wait_send()


def write_out(parts, *refs):
    ins, outs, (scratch, sem) = refs[:4], refs[4:9], refs[9:]
    size = ins[0].shape[0] // parts
    copies = [
        pltpu.make_async_copy(
            ins[m].at[pl.ds(i * size, size)], outs[m].at[pl.ds(i * size, size)], sem.at[m * parts + i]
        )
        for i in range(parts)
        for m in range(2)
    ]
    copies += [pltpu.make_async_copy(ins[2].at[m], outs[2 + m], sem.at[2 * parts + m]) for m in range(2)]
    for c in copies:
        c.start()
    scratch[...] = ins[3][...].astype(jnp.bfloat16)
    last = pltpu.make_async_copy(scratch, outs[4], sem.at[2 * parts + 2])
    last.start()
    for c in copies + [last]:
        c.wait()


def per_device(weight_gate, low_gate, high_gate, weight_up, low_up, high_up, norm_train, norm_step):
    devices, ny = lax.axis_size("zero"), lax.axis_size("cols")
    nz = devices // 2
    rows, columns = weight_gate.shape
    rank = low_gate.shape[1]
    share = norm_train.shape[0]
    tiles = columns // LANES
    f32, bf16 = jnp.float32, jnp.bfloat16
    hbm = pl.BlockSpec(memory_space=pltpu.HBM)
    vmem = pl.BlockSpec(memory_space=pltpu.VMEM)
    dma = pltpu.SemaphoreType.DMA
    serving_gate, serving_up, column, norm = pl.pallas_call(
        functools.partial(kernel, nz, ny),
        out_shape=(
            pltpu.VMEM((devices * rows, columns), bf16),
            pltpu.VMEM((devices * rows, columns), bf16),
            pltpu.VMEM((2, tiles, LANES), f32),
            pltpu.VMEM((devices, LANES), f32),
        ),
        in_specs=[hbm] * 8,
        out_specs=(vmem,) * 4,
        scratch_shapes=[
            pltpu.VMEM((2, rows, columns), bf16),
            pltpu.VMEM((2, rank, rows), bf16),
            pltpu.VMEM((2, rank, columns), bf16),
            pltpu.VMEM((2, 1, share), f32),
            pltpu.VMEM((2, 2, rows, columns), bf16),
            pltpu.VMEM((2, 2, rank, rows), bf16),
            pltpu.VMEM((2, rows, columns), f32),
            pltpu.VMEM((2, tiles, LANES), f32),
            pltpu.VMEM((tiles, LANES), f32),
            pltpu.VMEM((tiles, LANES), f32),
            pltpu.VMEM((tiles, LANES), f32),
            pltpu.VMEM((4, tiles, LANES), f32),
            pltpu.VMEM((2, 1, columns), f32),
            pltpu.VMEM((ny, 1, LANES), f32),
            pltpu.VMEM((2, nz, 1, LANES), f32),
            dma((8,)),
            dma((2, DEPTH)),
            dma((2, (nz - 1) * CH)),
            dma((2, 2)),
            dma((2, 2)),
            dma((2,)),
            dma((2,)),
            dma,
            dma((2, nz)),
            dma((nz + 1,)),
            dma((nz + 1,)),
            dma((2, ny - 1)),
            dma((2, ny - 1)),
            dma((nz,)),
            dma((nz,)),
            pltpu.SemaphoreType.REGULAR((2,)),
            pltpu.SemaphoreType.REGULAR((4,)),
        ],
        compiler_params=pltpu.CompilerParams(
            collective_id=0, has_side_effects=True, vmem_limit_bytes=47 << 20
        ),
    )(
        weight_gate, low_gate.T, high_gate, weight_up, low_up.T, high_up,
        norm_train.reshape(1, share), norm_step.reshape(1, share),
    )
    parts = 4
    serving_gate, serving_up, column_gate, column_up, norm = pl.pallas_call(
        functools.partial(write_out, parts),
        out_shape=(
            jax.ShapeDtypeStruct((devices * rows, columns), bf16),
            jax.ShapeDtypeStruct((devices * rows, columns), bf16),
            jax.ShapeDtypeStruct((tiles, LANES), f32),
            jax.ShapeDtypeStruct((tiles, LANES), f32),
            jax.ShapeDtypeStruct((devices, LANES), bf16),
        ),
        in_specs=[vmem] * 4,
        out_specs=(hbm,) * 5,
        scratch_shapes=[pltpu.VMEM((devices, LANES), bf16), dma((2 * parts + 3,))],
        compiler_params=pltpu.CompilerParams(vmem_limit_bytes=20 << 20),
    )(serving_gate, serving_up, column, norm)
    return (serving_gate, serving_up, column_gate.reshape(-1), column_up.reshape(-1), norm.reshape(-1))


def solution(mesh):
    in_specs = (
        P(("job", "zero"), "cols"),
        P(("job", "zero"), None),
        P("job", "cols"),
        P(("job", "zero"), "cols"),
        P(("job", "zero"), None),
        P("job", "cols"),
        P(("job", "zero", "cols")),
        P(("job", "zero", "cols")),
    )
    out_specs = (
        P("job", "cols"),
        P("job", "cols"),
        P(("job", "cols")),
        P(("job", "cols")),
        P("job"),
    )
    return jax.shard_map(
        per_device, mesh=mesh, in_specs=in_specs, out_specs=out_specs, check_vma=False
    )
```
